128 devices in a mesh: rep: 1, dp: 128 (over x, y, z, core).
Axes of the slice: x: 4, y: 4, z: 4, core: 2. Of those that a mesh axis runs over, the one named last changes fastest.
Arguments:
- g_w_gate: bfloat16 [128, 2, 1024, 2816], P(('rep', 'dp'))
- g_w_up: bfloat16 [128, 2, 1024, 2816], P(('rep', 'dp'))
- g_w_down: bfloat16 [128, 2, 2816, 1024], P(('rep', 'dp'))
- w_gate: bfloat16 [2, 1024, 2816], replicated
- w_up: bfloat16 [2, 1024, 2816], replicated
- w_down: bfloat16 [2, 2816, 1024], replicated
- m_w_gate: float32 [2, 1024, 2816], P(None, 'dp')
- m_w_up: float32 [2, 1024, 2816], P(None, 'dp')
- m_w_down: float32 [2, 2816, 1024], P(None, 'dp')
- v_w_gate: float32 [2, 1024, 2816], P(None, 'dp')
- v_w_up: float32 [2, 1024, 2816], P(None, 'dp')
- v_w_down: float32 [2, 2816, 1024], P(None, 'dp')
Outputs:
- output 1: bfloat16 [2, 1024, 2816], P('rep')
- output 2: bfloat16 [2, 1024, 2816], P('rep')
- output 3: bfloat16 [2, 2816, 1024], P('rep')
- output 4: float32 [2, 1024, 2816], P('rep', 'dp')
- output 5: float32 [2, 1024, 2816], P('rep', 'dp')
- output 6: float32 [2, 2816, 1024], P('rep', 'dp')
- output 7: float32 [2, 1024, 2816], P('rep', 'dp')
- output 8: float32 [2, 1024, 2816], P('rep', 'dp')
- output 9: float32 [2, 2816, 1024], P('rep', 'dp')
All inputs are finite; a program needn't handle non-finite values.
Results may differ from the reference program's by a relative error of at most 0.022.
Values are sent between devices in bfloat16 or wider.
A program may use at most 1.5 GiB of HBM per device.

```python
import jax
import jax.numpy as jnp
from jax import lax

DEVICES = 128
D = 1024
FF = 2816
LAYERS = 2
NAMES = ("w_gate", "w_up", "w_down")
SHAPES = {"w_gate": (LAYERS, D, FF), "w_up": (LAYERS, D, FF), "w_down": (LAYERS, FF, D)}


def setup_inputs(seed: int = 0, part: int = 0) -> dict:
    kz, *keys = jax.random.split(jax.random.key(seed), 1 + 5 * len(NAMES))
    loud = 2.0 ** jax.random.uniform(kz, (), jnp.float32, -1.0, 1.0)
    drawn = {}
    for name, key, both in zip(NAMES, keys[:3], keys[3:6], strict=True):
        own = jax.random.normal(jax.random.fold_in(key, part), (DEVICES, *SHAPES[name]), jnp.float32)
        shared = jax.random.normal(jax.random.fold_in(both, part), SHAPES[name], jnp.float32)
        drawn["g_" + name] = (loud * (0.7 * shared / DEVICES + 0.7 * own * DEVICES**-0.5)).astype(jnp.bfloat16)
    for name, key in zip(NAMES, keys[6:9], strict=True):
        drawn[name] = (jax.random.normal(key, SHAPES[name], jnp.float32) * SHAPES[name][1] ** -0.5).astype(jnp.bfloat16)
    for name, key in zip(NAMES, keys[9:12], strict=True):
        drawn["m_" + name] = loud * 0.5 * jax.random.normal(key, SHAPES[name], jnp.float32)
    for name, key in zip(NAMES, keys[12:15], strict=True):
        drawn["v_" + name] = loud * loud * jax.random.uniform(key, SHAPES[name], jnp.float32, 0.5, 1.5)
    return drawn


def adamw(w, m, v, g):
    m = 0.9 * m + 0.1 * g
    v = 0.95 * v + 0.05 * g * g
    step = m * lax.rsqrt(v + 1e-8) + 0.1 * w
    return (w - 0.02 * step).astype(jnp.bfloat16), m, v


def clipped(gradients, sum_of_squares, count):
    factor = jnp.minimum(1.0, 0.5 * lax.rsqrt(sum_of_squares / count + 1e-30))
    return [g * factor for g in gradients]


def reference(g_w_gate, g_w_up, g_w_down, w_gate, w_up, w_down, m_w_gate, m_w_up, m_w_down, v_w_gate, v_w_up, v_w_down):
    def total(terms):
        return lax.scan(lambda so_far, term: (so_far + term.astype(jnp.float32), None), jnp.zeros(terms.shape[1:], jnp.float32), terms)[0]

    gradients = [total(terms).astype(jnp.bfloat16).astype(jnp.float32) for terms in (g_w_gate, g_w_up, g_w_down)]
    gradients = clipped(gradients, sum(jnp.sum(g * g) for g in gradients), sum(g.size for g in gradients))
    new = [
        adamw(w.astype(jnp.float32), m, v, g)
        for w, m, v, g in zip((w_gate, w_up, w_down), (m_w_gate, m_w_up, m_w_down), (v_w_gate, v_w_up, v_w_down), gradients, strict=True)
    ]
    return tuple(one[which] for which in range(3) for one in new)
```

```python
import functools

import jax
import jax.numpy as jnp
from jax import lax
from jax.experimental import pallas as pl
from jax.experimental.pallas import tpu as pltpu
from jax.sharding import PartitionSpec as P

MESH = pl.DeviceIdType.MESH
F32, BF16 = jnp.float32, jnp.bfloat16
AXES = ((0, 1, 2), (1, 2, 0), (2, 0, 1))
LAYERS = 2
EACH, SIDES, PLACES, OTHERS, LANDED = range(3), range(2), range(4), range(1, 4), range(2, 6)
AHEAD, BEHIND = (1, 3), (3, 1)


def order(j):
    return lax.rem(2 + j + (j // 2) * (2 * j - 3), 4)


def loop(body, n=4):
    lax.fori_loop(0, n, lambda j, c: (body(j), c)[1], 0)


def f32(x):
    return x.astype(F32)


def step_kernel(
    count, gg, gu, gd, wg, wu, wd, mg, mu, md, vg, vu, vd,
    Wg, Wu, Wd, mg2, mu2, md2, vg2, vu2, vd2,
    R1g, R1u, R1d, R2g, R2u, R2d, Q1g, Q1u, Q1d, Q2g, Q2u, Q2d, P1g, P1u, P1d, P2g, P2u, P2d,
    own_g, own_u, own_d, quad_g, rows, new_rows, cols, norms,
    load_sem, own_sem, d2d_s, d2d_r, a_s, a_r, b_s, b_r, c_s, c_r, x_s, x_r, n_s, n_r,
):
    g_in, W, w_in = (gg, gu, gd), (Wg, Wu, Wd), (wg, wu, wd)
    R1, R2, Q1, Q2, P1, P2 = (R1g, R1u, R1d), (R2g, R2u, R2d), (Q1g, Q1u, Q1d), (Q2g, Q2u, Q2d), (P1g, P1u, P1d), (P2g, P2u, P2d)
    quarter = cols.shape[-1]
    me = lax.axis_index("dp")
    k = lax.rem(me, 2)
    pos = (me // 32, lax.rem(me // 8, 4), lax.rem(me // 2, 4))
    q = lax.rem(me, 4)

    def device(p, core):
        return ((p[0] * 4 + p[1]) * 4 + p[2]) * 2 + core

    def near(axis, by):
        return device([lax.rem(c + by, 4) if n == axis else c for n, c in enumerate(pos)], k)

    partner = device(pos, 1 - k)
    quad = [me - q + lax.rem(q + by, 4) for by in OTHERS]

    def copy(src, dst, send, recv, to):
        return pltpu.make_async_remote_copy(src_ref=src, dst_ref=dst, send_sem=send, recv_sem=recv, device_id={"dp": to}, device_id_type=MESH)

    def at(i, l, a, b, c, core):
        place = dict(zip(AXES[i], (a, b, c)))
        return W[i].at[l, place[0], place[1], place[2], core]

    ALL = slice(None)
    home = [[pos[n] for n in AXES[i]] for i in EACH]

    def rel(i, which, by):
        return lax.rem(home[i][which] + by, 4)

    def source(i, a, b, core):
        if i == 0:
            return gg.at[:, a, b, :, core]
        if i == 1:
            return gu.at[:, :, a, b, core]
        columns = pl.ds(pl.multiple_of(lax.rem(a, 2) * (2 * quarter) + core * quarter, quarter), quarter)
        return gd.at[:, b, :, a // 2, :, :, columns]

    def load(i, ra, rb):
        a, b = rel(i, 0, ra), rel(i, 1, rb)
        return pltpu.make_async_copy(source(i, a, b, k), at(i, ALL, a, b, ALL, k), load_sem.at[i, ra, rb])

    def trade(i, ra, rb):
        a, b = rel(i, 0, ra), rel(i, 1, rb)
        return copy(source(i, a, b, 1 - k), at(i, ALL, a, b, ALL, k), d2d_s.at[i, ra, rb], d2d_r.at[i, ra, rb], partner)

    def traded(i, ra, rb):
        a, b = rel(i, 0, ra), rel(i, 1, rb)
        load(i, ra, rb).wait()
        copy(at(i, ALL, a, b, ALL, 1 - k), at(i, ALL, a, b, ALL, 1 - k), d2d_s.at[i, ra, rb], d2d_r.at[i, ra, rb], partner).wait_recv()

    across = me - q + (2 - 2 * (q // 2)) + (1 - k)
    peers = [partner, across] + [near(axis, by) for axis in EACH for by in OTHERS]
    barrier = pltpu.get_barrier_semaphore()
    for peer in peers:
        pl.semaphore_signal(barrier, inc=1, device_id={"dp": peer}, device_id_type=MESH)

    for ras in ((2,), (1, 3), (0,)):
        def start_loads(j, ras=ras):
            for ra in ras:
                for i in EACH:
                    load(i, ra, order(j)).start()
        if ras == (2,):
            loop(start_loads)
            pl.semaphore_wait(barrier, len(peers))
        else:
            loop(start_loads)
        def start_trades(j, ras=ras):
            for ra in ras:
                for i in EACH:
                    trade(i, ra, order(j)).start()
        loop(start_trades)
    own = [
        pltpu.make_async_copy(wg.at[:, pos[0], pos[1], pos[2], k], own_g, own_sem.at[0]),
        pltpu.make_async_copy(wu.at[:, pos[0], pos[1], pos[2], k], own_u, own_sem.at[1]),
        pltpu.make_async_copy(wd.at[:, pos[0], pos[1], pos[2] // 2], own_d, own_sem.at[2]),
    ]
    for n, (moment, there) in enumerate(zip((mg, mu, md, vg, vu, vd), (mg2, mu2, md2, vg2, vu2, vd2))):
        own.append(pltpu.make_async_copy(moment, there, own_sem.at[3 + n]))
    for one in own:
        one.start()

    def sum0(i, l, a, b, c):
        return f32(at(i, l, a, b, c, k)[...]) + f32(at(i, l, a, b, c, 1 - k)[...])

    def sum1(i, l, b, c):
        return sum0(i, l, home[i][0], b, c) + f32(R2[i][0, l, b, c]) + f32(R2[i][1, l, b, c])

    def sum2(i, l, c):
        return sum1(i, l, home[i][1], c) + f32(Q2[i][0, l, c]) + f32(Q2[i][1, l, c])

    def sum3(i, l):
        return sum2(i, l, home[i][2]) + f32(P2[i][0, l]) + f32(P2[i][1, l])

    def hop_a(i, kind, rb):
        d, b = kind % 2, rel(i, 1, rb)
        to = near(AXES[i][0], AHEAD[d])
        if kind < 2:
            src, dst = at(i, d, rel(i, 0, 2), b, ALL, k), R1[i].at[d, b]
        elif kind < 4:
            src, dst = at(i, 1 - d, rel(i, 0, AHEAD[d]), b, ALL, k), R2[i].at[d, 1 - d, b]
        else:
            src, dst = R1[i].at[d, b], R2[i].at[d, d, b]
        return copy(src, dst, a_s.at[i, kind, rb], a_r.at[i, kind, rb], to)

    def hop_b(i, kind):
        d = kind % 2
        to = near(AXES[i][1], AHEAD[d])
        if kind < 2:
            src, dst = R2[i].at[0, d, rel(i, 1, 2)], Q1[i].at[d]
        elif kind < 4:
            src, dst = R2[i].at[0, 1 - d, rel(i, 1, AHEAD[d])], Q2[i].at[d, 1 - d]
        else:
            src, dst = Q1[i].at[d], Q2[i].at[d, d]
        return copy(src, dst, b_s.at[i, kind], b_r.at[i, kind], to)

    def hop_c(i, kind):
        d = kind % 2
        to = near(AXES[i][2], AHEAD[d])
        if kind < 2:
            src, dst = Q2[i].at[0, d, rel(i, 2, 2)], P1[i].at[d]
        elif kind < 4:
            src, dst = Q2[i].at[0, 1 - d, rel(i, 2, AHEAD[d])], P2[i].at[d, 1 - d]
        else:
            src, dst = P1[i].at[d], P2[i].at[d, d]
        return copy(src, dst, c_s.at[i, kind], c_r.at[i, kind], to)

    def farthest(j):
        rb = order(j)
        for i in EACH:
            traded(i, 2, rb)
            a, b = rel(i, 0, 2), rel(i, 1, rb)

            def add(t):
                at(i, t // 4, a, b, lax.rem(t, 4), k)[...] = sum0(i, t // 4, a, b, lax.rem(t, 4)).astype(BF16)

            loop(add, 8)
            hop_a(i, 0, rb).start()
            hop_a(i, 1, rb).start()

    loop(farthest)

    def plain(j):
        rb = order(j)
        for i in EACH:
            for d in SIDES:
                ra = AHEAD[d]
                traded(i, ra, rb)
                a, b = rel(i, 0, ra), rel(i, 1, rb)

                def add(c):
                    at(i, 1 - d, a, b, c, k)[...] = sum0(i, 1 - d, a, b, c).astype(BF16)

                loop(add)
                hop_a(i, 2 + d, rb).start()

    loop(plain)

    def onward(j):
        rb = order(j)
        for i in EACH:
            for d in SIDES:
                hop_a(i, d, rb).wait_recv()
                a, b = rel(i, 0, AHEAD[d]), rel(i, 1, rb)

                def add(c):
                    R1[i][d, b, c] = (f32(R1[i][d, b, c]) + sum0(i, d, a, b, c)).astype(BF16)

                loop(add)
                hop_a(i, 4 + d, rb).start()

    loop(onward)

    def arrived_a(i, rb):
        traded(i, 0, rb)
        for kind in LANDED:
            hop_a(i, kind, rb).wait_recv()

    def settle_a(i, l, rb):
        b = rel(i, 1, rb)

        def add(c):
            R2[i][0, l, b, c] = sum1(i, l, b, c).astype(BF16)

        loop(add)

    for i in EACH:
        arrived_a(i, 2)
        for d in SIDES:
            settle_a(i, d, 2)
            hop_b(i, d).start()
    for rb, d in ((3, 1), (1, 0)):
        for i in EACH:
            arrived_a(i, rb)
            settle_a(i, 1 - d, rb)
            hop_b(i, 2 + d).start()
    for i in EACH:
        for d in SIDES:
            hop_b(i, d).wait_recv()
            b = rel(i, 1, AHEAD[d])

            def add(c, i=i, d=d, b=b):
                Q1[i][d, c] = (f32(Q1[i][d, c]) + sum1(i, d, b, c)).astype(BF16)

            loop(add)
            hop_b(i, 4 + d).start()

    for i in EACH:
        arrived_a(i, 0)
    for i in EACH:
        for kind in LANDED:
            hop_b(i, kind).wait_recv()
        for d in SIDES:
            c = rel(i, 2, 2)
            Q2[i][0, d, c] = sum2(i, d, c).astype(BF16)
            hop_c(i, d).start()
        for d in SIDES:
            c = rel(i, 2, AHEAD[d])
            Q2[i][0, 1 - d, c] = sum2(i, 1 - d, c).astype(BF16)
            hop_c(i, 2 + d).start()
    for i in EACH:
        for d in SIDES:
            hop_c(i, d).wait_recv()
            P1[i][d] = (f32(P1[i][d]) + sum2(i, d, rel(i, 2, AHEAD[d]))).astype(BF16)
            hop_c(i, 4 + d).start()
    squares = jnp.zeros((8, 128), F32)
    for i in (2, 0, 1):
        for kind in LANDED:
            hop_c(i, kind).wait_recv()
        for l in SIDES:
            total = sum3(i, l).astype(BF16)
            if i == 2:
                quad_g[q, l] = total
            else:
                P2[i][0, l] = total
            s = f32(total)
            s = s * s
            if i == 2:
                s = jnp.sum(s, axis=0)
            for lane in range(0, s.shape[-1], 128):
                squares = squares + s[:, lane : lane + 128]
        if i == 2:
            for n in EACH:
                copy(quad_g.at[q], quad_g.at[q], x_s.at[n], x_r.at[n], quad[n]).start()
    norms[0, 0] = squares

    def drain(j):
        for i in EACH:
            for kind in range(6):
                hop_a(i, kind, j).wait_send()
            for ra in PLACES:
                trade(i, ra, j).wait_send()

    loop(drain)
    for i in EACH:
        for kind in range(6):
            hop_b(i, kind).wait_send()
            hop_c(i, kind).wait_send()

    first = copy(norms.at[0, 0], norms.at[0, 1], n_s.at[0, 1], n_r.at[0, 1], partner)
    first.start()
    first.wait()
    norms[1, 0] = norms[0, 0] + norms[0, 1]
    for turn, axis in ((1, 2), (2, 1), (3, 0)):
        hops = [copy(norms.at[turn, 0], norms.at[turn, by], n_s.at[turn, by], n_r.at[turn, by], near(axis, by)) for by in OTHERS]
        for hop in hops:
            hop.start()
        for hop in hops:
            hop.wait()
        norms[turn + 1, 0] = (norms[turn, 0] + norms[turn, 1]) + (norms[turn, 2] + norms[turn, 3])
    squares = norms[4, 0]
    squares = jnp.sum(jnp.sum(squares, axis=1, keepdims=True), axis=0, keepdims=True)
    factor = jnp.minimum(1.0, 0.5 * lax.rsqrt(squares / count + 1e-30))

    def adamw(w, m, v, g):
        g = g * factor
        m = 0.9 * m + 0.1 * g
        v = 0.95 * v + 0.05 * g * g
        step = m * lax.rsqrt(v + 1e-8) + 0.1 * w
        return (w - 0.02 * step).astype(BF16), m, v

    for one in own:
        one.wait()
    for n in EACH:
        copy(quad_g.at[q], quad_g.at[q], x_s.at[n], x_r.at[n], quad[n]).wait_send()
        theirs = quad_g.at[lax.rem(q + n + 1, 4)]
        copy(theirs, theirs, x_s.at[2 - n], x_r.at[2 - n], quad[n]).wait_recv()
    n_rows = md.shape[0]
    for l in SIDES:
        for n in PLACES:
            rows[0, :, n * quarter : (n + 1) * quarter] = f32(quad_g[n, l]).reshape(4 * n_rows, quarter)
        rows[1] = f32(own_d[l]).reshape(4 * n_rows, 4 * quarter)
        for n in PLACES:

            @pl.when(q == n)
            def _():
                mine = slice(n * n_rows, (n + 1) * n_rows)
                new, m, v = adamw(rows[1, mine, :], md2[:, l, :], vd2[:, l, :], rows[0, mine, :])
                new_rows[l] = new
                md2[:, l, :] = m
                vd2[:, l, :] = v
                cols[n, l] = new[:, n * quarter : (n + 1) * quarter]

    def piece(n):
        to = lax.rem(q + n + 1, 4)
        return new_rows.at[:, :, pl.ds(pl.multiple_of(to * quarter, quarter), quarter)]

    for n in EACH:
        copy(piece(n), cols.at[q], x_s.at[3 + n], x_r.at[3 + n], quad[n]).start()

    for i, own_w, m_ref, v_ref in ((0, own_g, mg2, vg2), (1, own_u, mu2, vu2)):
        for l in SIDES:
            new, m_ref[l], v_ref[l] = adamw(f32(own_w[l]), m_ref[l], v_ref[l], f32(P2[i][0, l]))
            at(i, l, *home[i], k)[...] = new

    def back_c(i, kind):
        d = kind % 2
        a, b, c = home[i]
        if kind < 2:
            ref = at(i, ALL, a, b, c, k)
        else:
            ref = at(i, d, a, b, rel(i, 2, BEHIND[d]), k)
        return copy(ref, ref, c_s.at[i, kind], c_r.at[i, kind], near(AXES[i][2], AHEAD[d]))

    def came_c(i, kind):
        d = kind % 2
        a, b, _ = home[i]
        ref = at(i, ALL, a, b, rel(i, 2, BEHIND[d]), k) if kind < 2 else at(i, d, a, b, rel(i, 2, 2), k)
        copy(ref, ref, c_s.at[i, kind], c_r.at[i, kind], partner).wait_recv()

    def back_b(i, kind):
        d = kind % 2
        a, b, _ = home[i]
        if kind < 2:
            ref = at(i, ALL, a, b, ALL, k)
        else:
            ref = at(i, d, a, rel(i, 1, BEHIND[d]), ALL, k)
        return copy(ref, ref, b_s.at[i, kind], b_r.at[i, kind], near(AXES[i][1], AHEAD[d]))

    def came_b(i, kind):
        d = kind % 2
        ref = at(i, ALL, home[i][0], rel(i, 1, BEHIND[d]), ALL, k) if kind < 2 else at(i, d, home[i][0], rel(i, 1, 2), ALL, k)
        copy(ref, ref, b_s.at[i, kind], b_r.at[i, kind], partner).wait_recv()

    def back_a(i, kind, rb):
        d, b = kind % 2, rel(i, 1, rb)
        if kind < 2:
            ref = at(i, ALL, home[i][0], b, ALL, k)
        else:
            ref = at(i, d, rel(i, 0, BEHIND[d]), b, ALL, k)
        return copy(ref, ref, a_s.at[i, kind, rb], a_r.at[i, kind, rb], near(AXES[i][0], AHEAD[d]))

    def came_a(i, kind, rb):
        d, b = kind % 2, rel(i, 1, rb)
        ref = at(i, ALL, rel(i, 0, BEHIND[d]), b, ALL, k) if kind < 2 else at(i, d, rel(i, 0, 2), b, ALL, k)
        copy(ref, ref, a_s.at[i, kind, rb], a_r.at[i, kind, rb], partner).wait_recv()

    def share(i, ra, rb):
        ref = at(i, ALL, rel(i, 0, ra), rel(i, 1, rb), ALL, k)
        return copy(ref, ref, d2d_s.at[i, ra, rb], d2d_r.at[i, ra, rb], partner)

    def shared(i, ra, rb):
        ref = at(i, ALL, rel(i, 0, ra), rel(i, 1, rb), ALL, 1 - k)
        copy(ref, ref, d2d_s.at[i, ra, rb], d2d_r.at[i, ra, rb], partner).wait_recv()

    for i in (0, 1):
        for kind in SIDES:
            back_c(i, kind).start()
    for n in EACH:
        copy(piece(n), cols.at[q], x_s.at[3 + n], x_r.at[3 + n], quad[n]).wait_send()
        theirs = cols.at[lax.rem(q + n + 1, 4)]
        copy(theirs, theirs, x_s.at[5 - n], x_r.at[5 - n], quad[n]).wait_recv()
    for l in SIDES:
        for n in PLACES:
            rows[0, n * n_rows : (n + 1) * n_rows, 0:quarter] = f32(cols[n, l])
        at(2, l, *home[2], k)[...] = rows[0, :, 0:quarter].reshape(n_rows // 2, 8, quarter).astype(BF16)
    for kind in SIDES:
        back_c(2, kind).start()
    for i in EACH:
        for d in SIDES:
            came_c(i, d)
            back_c(i, 2 + d).start()
    for i in EACH:
        for d in SIDES:
            came_c(i, 2 + d)
        for kind in SIDES:
            back_b(i, kind).start()
    for i in EACH:
        for kind in SIDES:
            back_a(i, kind, 0).start()
        share(i, 0, 0).start()
    for i in EACH:
        for d in SIDES:
            came_b(i, d)
            back_b(i, 2 + d).start()
    for i in EACH:
        for rb in (3, 1):
            for kind in SIDES:
                back_a(i, kind, rb).start()
            share(i, 0, rb).start()
    for i in EACH:
        for d in SIDES:
            came_b(i, 2 + d)
        for kind in SIDES:
            back_a(i, kind, 2).start()
        share(i, 0, 2).start()

    def pass_on(j):
        rb = lax.rem(order(j) + 2, 4)
        for i in EACH:
            for d in SIDES:
                came_a(i, d, rb)
                back_a(i, 2 + d, rb).start()
                share(i, BEHIND[d], rb).start()

    loop(pass_on)

    def last(j):
        rb = lax.rem(order(j) + 2, 4)
        for i in EACH:
            for d in SIDES:
                came_a(i, 2 + d, rb)
            share(i, 2, rb).start()

    loop(last)

    def finish(j):
        for i in EACH:
            for ra in PLACES:
                shared(i, ra, j)
                share(i, ra, j).wait_send()
            for kind in PLACES:
                back_a(i, kind, j).wait_send()

    loop(finish)
    for i in EACH:
        for kind in PLACES:
            back_b(i, kind).wait_send()
            back_c(i, kind).wait_send()


def write_kernel(Wg, Wu, Wd, *refs):
    small_in, (og, ou, od), outs, sems = refs[:6], refs[6:9], refs[9:15], refs[15]
    quarter = Wd.shape[-1]
    copies = [pltpu.make_async_copy(Wg, og, sems.at[14]), pltpu.make_async_copy(Wu, ou, sems.at[15])]
    for n in PLACES:
        for zh in SIDES:
            copies.append(
                pltpu.make_async_copy(Wd.at[:, :, :, 2 * zh + n // 2, n % 2], od.at[:, :, :, zh, :, :, n * quarter : (n + 1) * quarter], sems.at[2 * n + zh])
            )
    for n in range(6):
        copies.append(pltpu.make_async_copy(small_in[n], outs[n], sems.at[8 + n]))
    for one in copies:
        one.start()
    for one in copies:
        one.wait()


def solution(mesh):
    def step(*arrays):
        terms, weights, m, v = (arrays[i : i + 3] for i in (0, 3, 6, 9))
        wide, tall = weights[0].shape[2], weights[2].shape[2]
        n_rows = m[2].shape[1]
        m, v = ([jnp.swapaxes(one, 0, 1) if n == 2 else one for n, one in enumerate(some)] for some in (m, v))
        whole = (LAYERS, 4, 4, 4, 2, 8, wide)
        whole_d = (LAYERS, 4, 4, 2, n_rows // 2, 8, tall)
        shapes = (whole, whole, whole_d)
        quarter = tall // 4
        units = ((8, wide), (8, wide), (n_rows // 2, 8, quarter))
        g = [t[0].reshape(s) for t, s in zip(terms, shapes)]
        w = [t.reshape(s) for t, s in zip(weights, shapes)]
        count = float(sum(one.size for one in weights))
        blocks = [pltpu.VMEM((LAYERS, 4, 4, 4, 2, *u), BF16) for u in units]
        moments = [pltpu.VMEM(one.shape, F32) for one in (*m, *v)]
        hbm, vmem = pl.BlockSpec(memory_space=pltpu.HBM), pl.BlockSpec(memory_space=pltpu.VMEM)
        dma = pltpu.SemaphoreType.DMA
        results = pl.pallas_call(
            functools.partial(step_kernel, count),
            out_shape=blocks + moments,
            in_specs=[hbm] * 12,
            out_specs=[vmem] * 9,
            scratch_shapes=[
                *[pltpu.VMEM((2, 4, 4, *u), BF16) for u in units],
                *[pltpu.VMEM((2, LAYERS, 4, 4, *u), BF16) for u in units],
                *[pltpu.VMEM((2, 4, *u), BF16) for u in units],
                *[pltpu.VMEM((2, LAYERS, 4, *u), BF16) for u in units],
                *[pltpu.VMEM((2, *u), BF16) for u in units],
                *[pltpu.VMEM((2, LAYERS, *u), BF16) for u in units],
                pltpu.VMEM((LAYERS, 8, wide), BF16),
                pltpu.VMEM((LAYERS, 8, wide), BF16),
                pltpu.VMEM((LAYERS, n_rows // 2, 8, tall), BF16),
                pltpu.VMEM((4, LAYERS, *units[2]), BF16),
                pltpu.VMEM((2, 4 * n_rows, tall), F32),
                pltpu.VMEM((LAYERS, n_rows, tall), BF16),
                pltpu.VMEM((4, LAYERS, n_rows, quarter), BF16),
                pltpu.VMEM((5, 4, 8, 128), F32),
                dma((3, 4, 4)), dma((9,)), dma((3, 4, 4)), dma((3, 4, 4)),
                dma((3, 6, 4)), dma((3, 6, 4)), dma((3, 6)), dma((3, 6)), dma((3, 6)), dma((3, 6)),
                dma((6,)), dma((6,)), dma((4, 4)), dma((4, 4)),
            ],
            compiler_params=pltpu.CompilerParams(collective_id=0, has_side_effects=True, vmem_limit_bytes=26600000),
            name="step",
        )(*g, *w, *m, *v)
        outs = [jax.ShapeDtypeStruct(s, BF16) for s in shapes] + [jax.ShapeDtypeStruct(one.shape, F32) for one in (*m, *v)]
        written = pl.pallas_call(
            write_kernel,
            out_shape=outs,
            in_specs=[vmem] * 9,
            out_specs=[hbm] * 9,
            scratch_shapes=[dma((16,))],
            compiler_params=pltpu.CompilerParams(vmem_limit_bytes=2**20),
            name="write",
        )(*results)
        new = [r.reshape(t.shape) for r, t in zip(written[:3], weights)]
        moved = [jnp.swapaxes(one, 0, 1) if n % 3 == 2 else one for n, one in enumerate(written[3:])]
        return (*new, *moved)

    all_of, cut = P(None, None, None), P(None, "dp", None)
    return jax.shard_map(
        step,
        mesh=mesh,
        in_specs=(P(("rep", "dp"), None, None, None),) * 3 + (all_of,) * 3 + (cut,) * 6,
        out_specs=(P("rep", None, None),) * 3 + (P("rep", "dp", None),) * 6,
        check_vma=False,
    )
```

```python
import functools

import jax
import jax.numpy as jnp
from jax import lax
from jax.experimental import pallas as pl
from jax.experimental.pallas import tpu as pltpu
from jax.sharding import PartitionSpec as P

MESH = pl.DeviceIdType.MESH
F32, BF16 = jnp.float32, jnp.bfloat16
AXES = ((0, 1, 2), (1, 2, 0), (2, 0, 1))
LAYERS = 2
EACH, SIDES, PLACES, OTHERS, LANDED = range(3), range(2), range(4), range(1, 4), range(2, 6)
AHEAD, BEHIND = (1, 3), (3, 1)


def order(j):
    return lax.rem(2 + j + (j // 2) * (2 * j - 3), 4)


def loop(body, n=4):
    lax.fori_loop(0, n, lambda j, c: (body(j), c)[1], 0)


def f32(x):
    return x.astype(F32)


def step_kernel(
    count, gg, gu, gd, wg, wu, wd, mg, mu, md, vg, vu, vd,
    Wg, Wu, Wd, mg2, mu2, md2, vg2, vu2, vd2,
    R1g, R1u, R1d, R2g, R2u, R2d, Q1g, Q1u, Q1d, Q2g, Q2u, Q2d, P1g, P1u, P1d, P2g, P2u, P2d,
    own_g, own_u, own_d, quad_g, rows, new_rows, cols, norms,
    load_sem, own_sem, d2d_s, d2d_r, a_s, a_r, b_s, b_r, c_s, c_r, x_s, x_r, n_s, n_r,
):
    g_in, W, w_in = (gg, gu, gd), (Wg, Wu, Wd), (wg, wu, wd)
    R1, R2, Q1, Q2, P1, P2 = (R1g, R1u, R1d), (R2g, R2u, R2d), (Q1g, Q1u, Q1d), (Q2g, Q2u, Q2d), (P1g, P1u, P1d), (P2g, P2u, P2d)
    quarter = cols.shape[-1]
    me = lax.axis_index("dp")
    k = lax.rem(me, 2)
    pos = (me // 32, lax.rem(me // 8, 4), lax.rem(me // 2, 4))
    q = lax.rem(me, 4)

    def device(p, core):
        return ((p[0] * 4 + p[1]) * 4 + p[2]) * 2 + core

    def near(axis, by):
        return device([lax.rem(c + by, 4) if n == axis else c for n, c in enumerate(pos)], k)

    partner = device(pos, 1 - k)
    quad = [me - q + lax.rem(q + by, 4) for by in OTHERS]

    def copy(src, dst, send, recv, to):
        return pltpu.make_async_remote_copy(src_ref=src, dst_ref=dst, send_sem=send, recv_sem=recv, device_id={"dp": to}, device_id_type=MESH)

    def at(i, l, a, b, c, core):
        place = dict(zip(AXES[i], (a, b, c)))
        return W[i].at[l, place[0], place[1], place[2], core]

    ALL = slice(None)
    home = [[pos[n] for n in AXES[i]] for i in EACH]

    def rel(i, which, by):
        return lax.rem(home[i][which] + by, 4)

    def source(i, a, b, core):
        if i == 0:
            return gg.at[:, a, b, :, core]
        if i == 1:
            return gu.at[:, :, a, b, core]
        columns = pl.ds(pl.multiple_of(lax.rem(a, 2) * (2 * quarter) + core * quarter, quarter), quarter)
        return gd.at[:, b, :, a // 2, :, :, columns]

    def load(i, ra, rb):
        a, b = rel(i, 0, ra), rel(i, 1, rb)
        return pltpu.make_async_copy(source(i, a, b, k), at(i, ALL, a, b, ALL, k), load_sem.at[i, ra, rb])

    def trade(i, ra, rb):
        a, b = rel(i, 0, ra), rel(i, 1, rb)
        return copy(source(i, a, b, 1 - k), at(i, ALL, a, b, ALL, k), d2d_s.at[i, ra, rb], d2d_r.at[i, ra, rb], partner)

    def traded(i, ra, rb):
        a, b = rel(i, 0, ra), rel(i, 1, rb)
        load(i, ra, rb).wait()
        copy(at(i, ALL, a, b, ALL, 1 - k), at(i, ALL, a, b, ALL, 1 - k), d2d_s.at[i, ra, rb], d2d_r.at[i, ra, rb], partner).wait_recv()

    across = me - q + (2 - 2 * (q // 2)) + (1 - k)
    peers = [partner, across] + [near(axis, by) for axis in EACH for by in AHEAD]
    barrier = pltpu.get_barrier_semaphore()
    for peer in peers:
        pl.semaphore_signal(barrier, inc=1, device_id={"dp": peer}, device_id_type=MESH)

    for ras in ((2,), (1, 3), (0,)):
        def start_loads(j, ras=ras):
            for ra in ras:
                for i in EACH:
                    load(i, ra, order(j)).start()
        if ras == (2,):
            loop(start_loads)
            pl.semaphore_wait(barrier, len(peers))
        else:
            loop(start_loads)
        def start_trades(j, ras=ras):
            for ra in ras:
                for i in EACH:
                    trade(i, ra, order(j)).start()
        loop(start_trades)
    own = [
        pltpu.make_async_copy(wg.at[:, pos[0], pos[1], pos[2], k], own_g, own_sem.at[0]),
        pltpu.make_async_copy(wu.at[:, pos[0], pos[1], pos[2], k], own_u, own_sem.at[1]),
        pltpu.make_async_copy(wd.at[:, pos[0], pos[1], pos[2] // 2], own_d, own_sem.at[2]),
    ]
    for n, (moment, there) in enumerate(zip((mg, mu, md, vg, vu, vd), (mg2, mu2, md2, vg2, vu2, vd2))):
        own.append(pltpu.make_async_copy(moment, there, own_sem.at[3 + n]))
    for one in own:
        one.start()

    def sum0(i, l, a, b, c):
        return f32(at(i, l, a, b, c, k)[...]) + f32(at(i, l, a, b, c, 1 - k)[...])

    def sum1(i, l, b, c):
        return sum0(i, l, home[i][0], b, c) + f32(R2[i][0, l, b, c]) + f32(R2[i][1, l, b, c])

    def sum2(i, l, c):
        return sum1(i, l, home[i][1], c) + f32(Q2[i][0, l, c]) + f32(Q2[i][1, l, c])

    def sum3(i, l):
        return sum2(i, l, home[i][2]) + f32(P2[i][0, l]) + f32(P2[i][1, l])

    def hop_a(i, kind, rb):
        d, b = kind % 2, rel(i, 1, rb)
        to = near(AXES[i][0], AHEAD[d])
        if kind < 2:
            src, dst = at(i, d, rel(i, 0, 2), b, ALL, k), R1[i].at[d, b]
        elif kind < 4:
            src, dst = at(i, 1 - d, rel(i, 0, AHEAD[d]), b, ALL, k), R2[i].at[d, 1 - d, b]
        else:
            src, dst = R1[i].at[d, b], R2[i].at[d, d, b]
        return copy(src, dst, a_s.at[i, kind, rb], a_r.at[i, kind, rb], to)

    def hop_b(i, kind):
        d = kind % 2
        to = near(AXES[i][1], AHEAD[d])
        if kind < 2:
            src, dst = R2[i].at[0, d, rel(i, 1, 2)], Q1[i].at[d]
        elif kind < 4:
            src, dst = R2[i].at[0, 1 - d, rel(i, 1, AHEAD[d])], Q2[i].at[d, 1 - d]
        else:
            src, dst = Q1[i].at[d], Q2[i].at[d, d]
        return copy(src, dst, b_s.at[i, kind], b_r.at[i, kind], to)

    def hop_c(i, kind):
        d = kind % 2
        to = near(AXES[i][2], AHEAD[d])
        if kind < 2:
            src, dst = Q2[i].at[0, d, rel(i, 2, 2)], P1[i].at[d]
        elif kind < 4:
            src, dst = Q2[i].at[0, 1 - d, rel(i, 2, AHEAD[d])], P2[i].at[d, 1 - d]
        else:
            src, dst = P1[i].at[d], P2[i].at[d, d]
        return copy(src, dst, c_s.at[i, kind], c_r.at[i, kind], to)

    def farthest(j):
        rb = order(j)
        for i in EACH:
            traded(i, 2, rb)
            a, b = rel(i, 0, 2), rel(i, 1, rb)

            def add(t):
                at(i, t // 4, a, b, lax.rem(t, 4), k)[...] = sum0(i, t // 4, a, b, lax.rem(t, 4)).astype(BF16)

            loop(add, 8)
            hop_a(i, 0, rb).start()
            hop_a(i, 1, rb).start()

    loop(farthest)

    def plain(j):
        rb = order(j)
        for i in EACH:
            for d in SIDES:
                ra = AHEAD[d]
                traded(i, ra, rb)
                a, b = rel(i, 0, ra), rel(i, 1, rb)

                def add(c):
                    at(i, 1 - d, a, b, c, k)[...] = sum0(i, 1 - d, a, b, c).astype(BF16)

                loop(add)
                hop_a(i, 2 + d, rb).start()

    loop(plain)

    def onward(j):
        rb = order(j)
        for i in EACH:
            for d in SIDES:
                hop_a(i, d, rb).wait_recv()
                a, b = rel(i, 0, AHEAD[d]), rel(i, 1, rb)

                def add(c):
                    R1[i][d, b, c] = (f32(R1[i][d, b, c]) + sum0(i, d, a, b, c)).astype(BF16)

                loop(add)
                hop_a(i, 4 + d, rb).start()

    loop(onward)

    def arrived_a(i, rb):
        traded(i, 0, rb)
        for kind in LANDED:
            hop_a(i, kind, rb).wait_recv()

    def settle_a(i, l, rb):
        b = rel(i, 1, rb)

        def add(c):
            R2[i][0, l, b, c] = sum1(i, l, b, c).astype(BF16)

        loop(add)

    for i in EACH:
        arrived_a(i, 2)
        for d in SIDES:
            settle_a(i, d, 2)
            hop_b(i, d).start()
    for rb, d in ((3, 1), (1, 0)):
        for i in EACH:
            arrived_a(i, rb)
            settle_a(i, 1 - d, rb)
            hop_b(i, 2 + d).start()
    for i in EACH:
        for d in SIDES:
            hop_b(i, d).wait_recv()
            b = rel(i, 1, AHEAD[d])

            def add(c, i=i, d=d, b=b):
                Q1[i][d, c] = (f32(Q1[i][d, c]) + sum1(i, d, b, c)).astype(BF16)

            loop(add)
            hop_b(i, 4 + d).start()

    for i in EACH:
        arrived_a(i, 0)
    for i in EACH:
        for kind in LANDED:
            hop_b(i, kind).wait_recv()
        for d in SIDES:
            c = rel(i, 2, 2)
            Q2[i][0, d, c] = sum2(i, d, c).astype(BF16)
            hop_c(i, d).start()
        for d in SIDES:
            c = rel(i, 2, AHEAD[d])
            Q2[i][0, 1 - d, c] = sum2(i, 1 - d, c).astype(BF16)
            hop_c(i, 2 + d).start()
    for i in EACH:
        for d in SIDES:
            hop_c(i, d).wait_recv()
            P1[i][d] = (f32(P1[i][d]) + sum2(i, d, rel(i, 2, AHEAD[d]))).astype(BF16)
            hop_c(i, 4 + d).start()
    squares = jnp.zeros((8, 128), F32)
    for i in (2, 0, 1):
        for kind in LANDED:
            hop_c(i, kind).wait_recv()
        for l in SIDES:
            total = sum3(i, l).astype(BF16)
            if i == 2:
                quad_g[q, l] = total
            else:
                P2[i][0, l] = total
            s = f32(total)
            s = s * s
            if i == 2:
                s = jnp.sum(s, axis=0)
            for lane in range(0, s.shape[-1], 128):
                squares = squares + s[:, lane : lane + 128]
        if i == 2:
            for n in EACH:
                copy(quad_g.at[q], quad_g.at[q], x_s.at[n], x_r.at[n], quad[n]).start()
    norms[0, 0] = jnp.sum(squares, axis=0, keepdims=True)

    def drain(j):
        for i in EACH:
            for kind in range(6):
                hop_a(i, kind, j).wait_send()
            for ra in PLACES:
                trade(i, ra, j).wait_send()

    loop(drain)
    for i in EACH:
        for kind in range(6):
            hop_b(i, kind).wait_send()
            hop_c(i, kind).wait_send()

    line, plane = lax.rem(me, 8), me // 8
    for turn, others in ((0, [plane * 8 + lax.rem(line + by, 8) for by in range(1, 8)]), (1, [lax.rem(plane + by, 16) * 8 + line for by in range(1, 16)])):
        hops = [copy(norms.at[turn, 0], norms.at[turn, by], n_s.at[turn, by], n_r.at[turn, by], to) for by, to in enumerate(others, 1)]
        for hop in hops:
            hop.start()
        for hop in hops:
            hop.wait()
        squares = jnp.sum(norms[turn, 0 : len(hops) + 1], axis=0)
        if turn == 0:
            norms[1, 0] = squares
    squares = jnp.sum(squares, axis=1, keepdims=True)
    factor = jnp.minimum(1.0, 0.5 * lax.rsqrt(squares / count + 1e-30))

    def adamw(w, m, v, g):
        g = g * factor
        m = 0.9 * m + 0.1 * g
        v = 0.95 * v + 0.05 * g * g
        step = m * lax.rsqrt(v + 1e-8) + 0.1 * w
        return (w - 0.02 * step).astype(BF16), m, v

    for one in own:
        one.wait()
    for n in EACH:
        copy(quad_g.at[q], quad_g.at[q], x_s.at[n], x_r.at[n], quad[n]).wait_send()
        theirs = quad_g.at[lax.rem(q + n + 1, 4)]
        copy(theirs, theirs, x_s.at[2 - n], x_r.at[2 - n], quad[n]).wait_recv()
    n_rows = md.shape[0]
    for l in SIDES:
        for n in PLACES:
            rows[0, :, n * quarter : (n + 1) * quarter] = f32(quad_g[n, l]).reshape(4 * n_rows, quarter)
        rows[1] = f32(own_d[l]).reshape(4 * n_rows, 4 * quarter)
        for n in PLACES:

            @pl.when(q == n)
            def _():
                mine = slice(n * n_rows, (n + 1) * n_rows)
                new, m, v = adamw(rows[1, mine, :], md2[:, l, :], vd2[:, l, :], rows[0, mine, :])
                new_rows[l] = new
                md2[:, l, :] = m
                vd2[:, l, :] = v
                cols[n, l] = new[:, n * quarter : (n + 1) * quarter]

    def piece(n):
        to = lax.rem(q + n + 1, 4)
        return new_rows.at[:, :, pl.ds(pl.multiple_of(to * quarter, quarter), quarter)]

    for n in EACH:
        copy(piece(n), cols.at[q], x_s.at[3 + n], x_r.at[3 + n], quad[n]).start()

    for i, own_w, m_ref, v_ref in ((0, own_g, mg2, vg2), (1, own_u, mu2, vu2)):
        for l in SIDES:
            new, m_ref[l], v_ref[l] = adamw(f32(own_w[l]), m_ref[l], v_ref[l], f32(P2[i][0, l]))
            at(i, l, *home[i], k)[...] = new

    def back_c(i, kind):
        d = kind % 2
        a, b, c = home[i]
        if kind < 2:
            ref = at(i, ALL, a, b, c, k)
        else:
            ref = at(i, d, a, b, rel(i, 2, BEHIND[d]), k)
        return copy(ref, ref, c_s.at[i, kind], c_r.at[i, kind], near(AXES[i][2], AHEAD[d]))

    def came_c(i, kind):
        d = kind % 2
        a, b, _ = home[i]
        ref = at(i, ALL, a, b, rel(i, 2, BEHIND[d]), k) if kind < 2 else at(i, d, a, b, rel(i, 2, 2), k)
        copy(ref, ref, c_s.at[i, kind], c_r.at[i, kind], partner).wait_recv()

    def back_b(i, kind):
        d = kind % 2
        a, b, _ = home[i]
        if kind < 2:
            ref = at(i, ALL, a, b, ALL, k)
        else:
            ref = at(i, d, a, rel(i, 1, BEHIND[d]), ALL, k)
        return copy(ref, ref, b_s.at[i, kind], b_r.at[i, kind], near(AXES[i][1], AHEAD[d]))

    def came_b(i, kind):
        d = kind % 2
        ref = at(i, ALL, home[i][0], rel(i, 1, BEHIND[d]), ALL, k) if kind < 2 else at(i, d, home[i][0], rel(i, 1, 2), ALL, k)
        copy(ref, ref, b_s.at[i, kind], b_r.at[i, kind], partner).wait_recv()

    def back_a(i, kind, rb):
        d, b = kind % 2, rel(i, 1, rb)
        if kind < 2:
            ref = at(i, ALL, home[i][0], b, ALL, k)
        else:
            ref = at(i, d, rel(i, 0, BEHIND[d]), b, ALL, k)
        return copy(ref, ref, a_s.at[i, kind, rb], a_r.at[i, kind, rb], near(AXES[i][0], AHEAD[d]))

    def came_a(i, kind, rb):
        d, b = kind % 2, rel(i, 1, rb)
        ref = at(i, ALL, rel(i, 0, BEHIND[d]), b, ALL, k) if kind < 2 else at(i, d, rel(i, 0, 2), b, ALL, k)
        copy(ref, ref, a_s.at[i, kind, rb], a_r.at[i, kind, rb], partner).wait_recv()

    def share(i, ra, rb):
        ref = at(i, ALL, rel(i, 0, ra), rel(i, 1, rb), ALL, k)
        return copy(ref, ref, d2d_s.at[i, ra, rb], d2d_r.at[i, ra, rb], partner)

    def shared(i, ra, rb):
        ref = at(i, ALL, rel(i, 0, ra), rel(i, 1, rb), ALL, 1 - k)
        copy(ref, ref, d2d_s.at[i, ra, rb], d2d_r.at[i, ra, rb], partner).wait_recv()

    def spread(i, c):
        a, b, _ = home[i]
        ref = at(i, ALL, a, b, c, k)
        for d in SIDES:
            copy(ref, ref, b_s.at[i, d], b_r.at[i, d], near(AXES[i][1], AHEAD[d])).start()
        for d in SIDES:
            copy(ref, ref, a_s.at[i, d, 0], a_r.at[i, d, 0], near(AXES[i][0], AHEAD[d])).start()

    def begin(i):
        for kind in SIDES:
            back_c(i, kind).start()
        spread(i, home[i][2])

    begin(0)
    begin(1)
    for n in EACH:
        copy(piece(n), cols.at[q], x_s.at[3 + n], x_r.at[3 + n], quad[n]).wait_send()
        theirs = cols.at[lax.rem(q + n + 1, 4)]
        copy(theirs, theirs, x_s.at[5 - n], x_r.at[5 - n], quad[n]).wait_recv()
    for l in SIDES:
        for n in PLACES:
            rows[0, n * n_rows : (n + 1) * n_rows, 0:quarter] = f32(cols[n, l])
        at(2, l, *home[2], k)[...] = rows[0, :, 0:quarter].reshape(n_rows // 2, 8, quarter).astype(BF16)
    begin(2)
    for i in EACH:
        for d in SIDES:
            came_c(i, d)
            back_c(i, 2 + d).start()
        for d in SIDES:
            spread(i, rel(i, 2, AHEAD[d]))
    for i in EACH:
        for d in SIDES:
            came_c(i, 2 + d)
        spread(i, rel(i, 2, 2))
        share(i, 0, 0).start()
    for i in EACH:
        for d in SIDES:
            came_b(i, d)
            back_b(i, 2 + d).start()
    for i in EACH:
        for rb in (3, 1):
            for kind in SIDES:
                back_a(i, kind, rb).start()
            share(i, 0, rb).start()
    for i in EACH:
        for d in SIDES:
            came_b(i, 2 + d)
        for kind in SIDES:
            back_a(i, kind, 2).start()
        share(i, 0, 2).start()

    def pass_on(j):
        rb = lax.rem(order(j) + 2, 4)
        for i in EACH:
            for d in SIDES:
                came_a(i, d, rb)
                back_a(i, 2 + d, rb).start()
                share(i, BEHIND[d], rb).start()

    loop(pass_on)

    def last(j):
        rb = lax.rem(order(j) + 2, 4)
        for i in EACH:
            for d in SIDES:
                came_a(i, 2 + d, rb)
            share(i, 2, rb).start()

    loop(last)

    def finish(j):
        for i in EACH:
            for ra in PLACES:
                shared(i, ra, j)
                share(i, ra, j).wait_send()
            for kind in PLACES:
                back_a(i, kind, j).wait_send()

    loop(finish)
    for i in EACH:
        for kind in PLACES:
            back_b(i, kind).wait_send()
            back_c(i, kind).wait_send()


def write_wide(W, out, *refs):
    one = pltpu.make_async_copy(W, out, refs[-1].at[0])
    one.start()
    one.wait()


def write_tall(n_small, W, *refs):
    small_in, out, small_out, sems = refs[:n_small], refs[n_small], refs[n_small + 1 : -1], refs[-1]
    quarter = W.shape[-1]
    copies = [pltpu.make_async_copy(r, o, sems.at[n]) for n, (r, o) in enumerate(zip(small_in, small_out))]
    for n in PLACES:
        for half in SIDES:
            columns = slice(n * quarter, (n + 1) * quarter)
            copies.append(pltpu.make_async_copy(W.at[:, :, :, 2 * half + n // 2, n % 2], out.at[:, :, :, half, :, :, columns], sems.at[len(copies)]))
    for one in copies:
        one.start()
    for one in copies:
        one.wait()


def solution(mesh):
    def step(*arrays):
        terms, weights, m, v = (arrays[i : i + 3] for i in (0, 3, 6, 9))
        wide, tall = weights[0].shape[2], weights[2].shape[2]
        n_rows = m[2].shape[1]
        m, v = ([jnp.swapaxes(one, 0, 1) if n == 2 else one for n, one in enumerate(some)] for some in (m, v))
        whole = (LAYERS, 4, 4, 4, 2, 8, wide)
        whole_d = (LAYERS, 4, 4, 2, n_rows // 2, 8, tall)
        shapes = (whole, whole, whole_d)
        quarter = tall // 4
        units = ((8, wide), (8, wide), (n_rows // 2, 8, quarter))
        g = [t[0].reshape(s) for t, s in zip(terms, shapes)]
        w = [t.reshape(s) for t, s in zip(weights, shapes)]
        count = float(sum(one.size for one in weights))
        blocks = [pltpu.VMEM((LAYERS, 4, 4, 4, 2, *u), BF16) for u in units]
        moments = [pltpu.VMEM(one.shape, F32) for one in (*m, *v)]
        hbm, vmem = pl.BlockSpec(memory_space=pltpu.HBM), pl.BlockSpec(memory_space=pltpu.VMEM)
        dma = pltpu.SemaphoreType.DMA
        results = pl.pallas_call(
            functools.partial(step_kernel, count),
            out_shape=blocks + moments,
            in_specs=[hbm] * 12,
            out_specs=[vmem] * 9,
            scratch_shapes=[
                *[pltpu.VMEM((2, 4, 4, *u), BF16) for u in units],
                *[pltpu.VMEM((2, LAYERS, 4, 4, *u), BF16) for u in units],
                *[pltpu.VMEM((2, 4, *u), BF16) for u in units],
                *[pltpu.VMEM((2, LAYERS, 4, *u), BF16) for u in units],
                *[pltpu.VMEM((2, *u), BF16) for u in units],
                *[pltpu.VMEM((2, LAYERS, *u), BF16) for u in units],
                pltpu.VMEM((LAYERS, 8, wide), BF16),
                pltpu.VMEM((LAYERS, 8, wide), BF16),
                pltpu.VMEM((LAYERS, n_rows // 2, 8, tall), BF16),
                pltpu.VMEM((4, LAYERS, *units[2]), BF16),
                pltpu.VMEM((2, 4 * n_rows, tall), F32),
                pltpu.VMEM((LAYERS, n_rows, tall), BF16),
                pltpu.VMEM((4, LAYERS, n_rows, quarter), BF16),
                pltpu.VMEM((2, 16, 1, 128), F32),
                dma((3, 4, 4)), dma((9,)), dma((3, 4, 4)), dma((3, 4, 4)),
                dma((3, 6, 4)), dma((3, 6, 4)), dma((3, 6)), dma((3, 6)), dma((3, 6)), dma((3, 6)),
                dma((6,)), dma((6,)), dma((2, 16)), dma((2, 16)),
            ],
            compiler_params=pltpu.CompilerParams(collective_id=0, has_side_effects=True, vmem_limit_bytes=26600000),
            name="step",
        )(*g, *w, *m, *v)

        def write(kernel, arrays, outs):
            return pl.pallas_call(
                kernel,
                out_shape=outs,
                in_specs=[vmem] * len(arrays),
                out_specs=[hbm] * len(outs),
                scratch_shapes=[dma((16,))],
                compiler_params=pltpu.CompilerParams(vmem_limit_bytes=2**20),
                name="write",
            )(*arrays)

        outs = [jax.ShapeDtypeStruct(s, BF16) for s in shapes]
        small = results[3:]
        new_gate, new_up = (write(write_wide, [r], [o])[0] for r, o in zip(results, outs[:2]))
        new_down, *moved = write(functools.partial(write_tall, len(small)), results[2:], outs[2:] + [jax.ShapeDtypeStruct(one.shape, F32) for one in small])
        new = [r.reshape(t.shape) for r, t in zip((new_gate, new_up, new_down), weights)]
        return (*new, *(jnp.swapaxes(one, 0, 1) if n % 3 == 2 else one for n, one in enumerate(moved)))

    all_of, cut = P(None, None, None), P(None, "dp", None)
    return jax.shard_map(
        step,
        mesh=mesh,
        in_specs=(P(("rep", "dp"), None, None, None),) * 3 + (all_of,) * 3 + (cut,) * 6,
        out_specs=(P("rep", None, None),) * 3 + (P("rep", "dp", None),) * 6,
        check_vma=False,
    )
```

```python
import functools

import jax
import jax.numpy as jnp
from jax import lax
from jax.experimental import pallas as pl
from jax.experimental.pallas import tpu as pltpu
from jax.sharding import PartitionSpec as P

MESH = pl.DeviceIdType.MESH
F32, BF16 = jnp.float32, jnp.bfloat16
AXES = ((0, 1, 2), (1, 2, 0), (2, 0, 1))
LAYERS = 2
A, B, C = range(3)
FAR = 2
EACH, SIDES, PLACES, OTHERS, LANDED = range(3), range(2), range(4), range(1, 4), range(2, 6)
AHEAD, BEHIND = (1, 3), (3, 1)


def order(j):
    return lax.rem(2 + j + (j // 2) * (2 * j - 3), 4)


def loop(body, n=4, start=0):
    lax.fori_loop(start, n, lambda j, c: (body(j), c)[1], 0)


def f32(x):
    return x.astype(F32)


def step_kernel(
    count, gg, gu, gd, wg, wu, wd, mg, mu, md, vg, vu, vd,
    Wg, Wu, Wd, mg2, mu2, md2, vg2, vu2, vd2,
    R1g, R1u, R1d, R2g, R2u, R2d, Q1g, Q1u, Q1d, Q2g, Q2u, Q2d, P1g, P1u, P1d, P2g, P2u, P2d,
    own_g, own_u, own_d, quad_g, rows, new_rows, cols, norms,
    load_sem, own_sem, d2d_s, d2d_r, a_s, a_r, b_s, b_r, c_s, c_r, x_s, x_r, n_s, n_r, piece_l, piece_r, tail_r,
):
    g_in, W, w_in = (gg, gu, gd), (Wg, Wu, Wd), (wg, wu, wd)
    R1, R2, Q1, Q2, P1, P2 = (R1g, R1u, R1d), (R2g, R2u, R2d), (Q1g, Q1u, Q1d), (Q2g, Q2u, Q2d), (P1g, P1u, P1d), (P2g, P2u, P2d)
    quarter = cols.shape[-1]
    me = lax.axis_index("dp")
    k = lax.rem(me, 2)
    pos = (me // 32, lax.rem(me // 8, 4), lax.rem(me // 2, 4))
    q = lax.rem(me, 4)

    def device(p, core):
        return ((p[0] * 4 + p[1]) * 4 + p[2]) * 2 + core

    def near(axis, by):
        return device([lax.rem(c + by, 4) if n == axis else c for n, c in enumerate(pos)], k)

    partner = device(pos, 1 - k)
    quad = [me - q + lax.rem(q + by, 4) for by in OTHERS]

    def copy(src, dst, send, recv, to):
        return pltpu.make_async_remote_copy(src_ref=src, dst_ref=dst, send_sem=send, recv_sem=recv, device_id={"dp": to}, device_id_type=MESH)

    def at(i, l, a, b, c, core):
        place = dict(zip(AXES[i], (a, b, c)))
        return W[i].at[l, place[0], place[1], place[2], core]

    ALL = slice(None)
    home = [[pos[n] for n in AXES[i]] for i in EACH]

    def rel(i, which, by):
        return lax.rem(home[i][which] + by, 4)

    def source(i, a, b, c, core):
        if i == 0:
            return gg.at[:, a, b, c, core]
        if i == 1:
            return gu.at[:, c, a, b, core]
        columns = pl.ds(pl.multiple_of(lax.rem(a, 2) * (2 * quarter) + core * quarter, quarter), quarter)
        return gd.at[:, b, c, a // 2, :, :, columns]

    def load(i, ra, rb):
        a, b = rel(i, A, ra), rel(i, B, rb)
        return pltpu.make_async_copy(source(i, a, b, ALL, k), at(i, ALL, a, b, ALL, k), load_sem.at[i, ra, rb])

    def trade(i, ra, rb):
        a, b = rel(i, A, ra), rel(i, B, rb)
        return copy(source(i, a, b, ALL, 1 - k), at(i, ALL, a, b, ALL, k), d2d_s.at[i, ra, rb], d2d_r.at[i, ra, rb], partner)

    def first_load(i, c):
        a, b = rel(i, A, FAR), rel(i, B, FAR)
        return pltpu.make_async_copy(source(i, a, b, c, k), at(i, ALL, a, b, c, k), piece_l.at[i, c])

    def first_trade(i, c):
        a, b = rel(i, A, FAR), rel(i, B, FAR)
        return copy(source(i, a, b, c, 1 - k), at(i, ALL, a, b, c, k), d2d_s.at[i, 2, 2], piece_r.at[i, c], partner)

    def first_traded(i, c):
        a, b = rel(i, A, FAR), rel(i, B, FAR)
        first_load(i, c).wait()
        ref = at(i, ALL, a, b, c, 1 - k)
        copy(ref, ref, d2d_s.at[i, 2, 2], piece_r.at[i, c], partner).wait_recv()

    def traded(i, ra, rb):
        a, b = rel(i, A, ra), rel(i, B, rb)
        load(i, ra, rb).wait()
        copy(at(i, ALL, a, b, ALL, 1 - k), at(i, ALL, a, b, ALL, 1 - k), d2d_s.at[i, ra, rb], d2d_r.at[i, ra, rb], partner).wait_recv()

    across = me - q + (2 - 2 * (q // 2)) + (1 - k)
    peers = [partner, across] + [near(axis, by) for axis in EACH for by in AHEAD]
    barrier = pltpu.get_barrier_semaphore()
    for peer in peers:
        pl.semaphore_signal(barrier, inc=1, device_id={"dp": peer}, device_id_type=MESH)

    def start_all(what, ras, start=0):
        def body(j):
            for ra in ras:
                for i in EACH:
                    what(i, ra, order(j)).start()

        loop(body, start=start)

    def start_first(what):
        def body(c):
            for i in EACH:
                what(i, c).start()

        loop(body)

    start_first(first_load)
    start_all(load, (2,), 1)
    pl.semaphore_wait(barrier, len(peers))
    start_first(first_trade)
    start_all(trade, (2,), 1)
    for ras in (AHEAD, (0,)):
        start_all(load, ras)
        start_all(trade, ras)
    own = [
        pltpu.make_async_copy(wg.at[:, pos[0], pos[1], pos[2], k], own_g, own_sem.at[0]),
        pltpu.make_async_copy(wu.at[:, pos[0], pos[1], pos[2], k], own_u, own_sem.at[1]),
        pltpu.make_async_copy(wd.at[:, pos[0], pos[1], pos[2] // 2], own_d, own_sem.at[2]),
    ]
    for n, (moment, there) in enumerate(zip((mg, mu, md, vg, vu, vd), (mg2, mu2, md2, vg2, vu2, vd2))):
        own.append(pltpu.make_async_copy(moment, there, own_sem.at[3 + n]))
    for one in own:
        one.start()

    def sum0(i, l, a, b, c):
        return f32(at(i, l, a, b, c, k)[...]) + f32(at(i, l, a, b, c, 1 - k)[...])

    def sum1(i, l, b, c):
        return sum0(i, l, home[i][0], b, c) + f32(R2[i][0, l, b, c]) + f32(R2[i][1, l, b, c])

    def sum2(i, l, c):
        return sum1(i, l, home[i][1], c) + f32(Q2[i][0, l, c]) + f32(Q2[i][1, l, c])

    def sum3(i, l):
        return sum2(i, l, home[i][2]) + f32(P2[i][0, l]) + f32(P2[i][1, l])

    def hop_a(i, kind, rb):
        d, b = kind % 2, rel(i, B, rb)
        to = near(AXES[i][0], AHEAD[d])
        if kind < 2:
            src, dst = at(i, d, rel(i, A, FAR), b, ALL, k), R1[i].at[d, b]
        elif kind < 4:
            src, dst = at(i, 1 - d, rel(i, A, AHEAD[d]), b, ALL, k), R2[i].at[d, 1 - d, b]
        else:
            src, dst = R1[i].at[d, b], R2[i].at[d, d, b]
        return copy(src, dst, a_s.at[i, kind, rb], a_r.at[i, kind, rb], to)

    def hop_b(i, kind, rc):
        d, c = kind % 2, rel(i, C, rc)
        to = near(AXES[i][1], AHEAD[d])
        if kind < 2:
            src, dst = R2[i].at[0, d, rel(i, B, FAR), c], Q1[i].at[d, c]
        elif kind < 4:
            src, dst = R2[i].at[0, 1 - d, rel(i, B, AHEAD[d]), c], Q2[i].at[d, 1 - d, c]
        else:
            src, dst = Q1[i].at[d, c], Q2[i].at[d, d, c]
        return copy(src, dst, b_s.at[i, kind, rc], b_r.at[i, kind, rc], to)

    def hop_c(i, kind):
        d = kind % 2
        to = near(AXES[i][2], AHEAD[d])
        if kind < 2:
            src, dst = Q2[i].at[0, d, rel(i, C, FAR)], P1[i].at[d]
        elif kind < 4:
            src, dst = Q2[i].at[0, 1 - d, rel(i, C, AHEAD[d])], P2[i].at[d, 1 - d]
        else:
            src, dst = P1[i].at[d], P2[i].at[d, d]
        return copy(src, dst, c_s.at[i, kind], c_r.at[i, kind], to)

    def farthest(j):
        rb = order(j)
        for i in EACH:
            traded(i, 2, rb)
            a, b = rel(i, A, FAR), rel(i, B, rb)

            def add(t):
                at(i, t // 4, a, b, lax.rem(t, 4), k)[...] = sum0(i, t // 4, a, b, lax.rem(t, 4)).astype(BF16)

            loop(add, 8)
            hop_a(i, 0, rb).start()
            hop_a(i, 1, rb).start()

    def farthest_first(c):
        for i in EACH:
            first_traded(i, c)
            a, b = rel(i, A, FAR), rel(i, B, FAR)
            for l in SIDES:
                ref = at(i, l, a, b, c, k)
                ref[...] = sum0(i, l, a, b, c).astype(BF16)
                copy(ref, R1[i].at[l, b, c], a_s.at[i, l, 2], a_r.at[i, l, 2], near(AXES[i][0], AHEAD[l])).start()

    loop(farthest_first)
    loop(farthest, start=1)

    def plain(j):
        rb = order(j)
        for i in EACH:
            for d in SIDES:
                ra = AHEAD[d]
                traded(i, ra, rb)
                a, b = rel(i, A, ra), rel(i, B, rb)

                def add(c):
                    at(i, 1 - d, a, b, c, k)[...] = sum0(i, 1 - d, a, b, c).astype(BF16)

                loop(add)
                hop_a(i, 2 + d, rb).start()

    loop(plain)

    def onward(j):
        rb = order(j)
        for i in EACH:
            for d in SIDES:
                hop_a(i, d, rb).wait_recv()
                a, b = rel(i, A, AHEAD[d]), rel(i, B, rb)

                def add(c):
                    R1[i][d, b, c] = (f32(R1[i][d, b, c]) + sum0(i, d, a, b, c)).astype(BF16)

                loop(add)
                hop_a(i, 4 + d, rb).start()

    loop(onward)

    def arrived_a(i, rb):
        traded(i, 0, rb)
        for kind in LANDED:
            hop_a(i, kind, rb).wait_recv()

    def settle_a(i, l, rb, rc):
        b, c = rel(i, B, rb), rel(i, C, rc)
        R2[i][0, l, b, c] = sum1(i, l, b, c).astype(BF16)

    for i in EACH:
        arrived_a(i, 2)

        def far_b(j, i=i):
            for d in SIDES:
                settle_a(i, d, 2, order(j))
                hop_b(i, d, order(j)).start()

        loop(far_b)
    for rb in AHEAD:
        for i in EACH:
            arrived_a(i, rb)

    def near_b(j):
        rc = order(j)
        for i in EACH:
            for d in SIDES:
                settle_a(i, 1 - d, AHEAD[d], rc)
                hop_b(i, 2 + d, rc).start()
        for i in EACH:
            for d in SIDES:
                hop_b(i, d, rc).wait_recv()
                c = rel(i, C, rc)
                Q1[i][d, c] = (f32(Q1[i][d, c]) + sum1(i, d, rel(i, B, AHEAD[d]), c)).astype(BF16)
                hop_b(i, 4 + d, rc).start()

    loop(near_b)
    for i in EACH:
        arrived_a(i, 0)

    def arrived_b(i, rc):
        for kind in LANDED:
            hop_b(i, kind, rc).wait_recv()

    for i in EACH:
        arrived_b(i, 2)
        for d in SIDES:
            c = rel(i, C, FAR)
            Q2[i][0, d, c] = sum2(i, d, c).astype(BF16)
            hop_c(i, d).start()
    for d in (1, 0):
        for i in EACH:
            arrived_b(i, AHEAD[d])
            c = rel(i, C, AHEAD[d])
            Q2[i][0, 1 - d, c] = sum2(i, 1 - d, c).astype(BF16)
            hop_c(i, 2 + d).start()
    for i in EACH:
        for d in SIDES:
            hop_c(i, d).wait_recv()
            P1[i][d] = (f32(P1[i][d]) + sum2(i, d, rel(i, C, AHEAD[d]))).astype(BF16)
            hop_c(i, 4 + d).start()
    for i in EACH:
        arrived_b(i, 0)
    squares = jnp.zeros((8, 128), F32)
    for i in (2, 0, 1):
        for kind in LANDED:
            hop_c(i, kind).wait_recv()
        for l in SIDES:
            total = sum3(i, l).astype(BF16)
            if i == 2:
                quad_g[q, l] = total
            else:
                P2[i][0, l] = total
            s = f32(total)
            s = s * s
            if i == 2:
                s = jnp.sum(s, axis=0)
            for lane in range(0, s.shape[-1], 128):
                squares = squares + s[:, lane : lane + 128]
        if i == 2:
            for n in EACH:
                copy(quad_g.at[q], quad_g.at[q], x_s.at[n], x_r.at[n], quad[n]).start()
    norms[0, 0] = jnp.sum(squares, axis=0, keepdims=True)

    def drain(j):
        for i in EACH:
            for kind in range(6):
                hop_a(i, kind, j).wait_send()
                hop_b(i, kind, j).wait_send()
            for ra in PLACES:
                trade(i, ra, j).wait_send()

    loop(drain)
    for i in EACH:
        for kind in range(6):
            hop_c(i, kind).wait_send()

    line, plane = lax.rem(me, 8), me // 8
    for turn, others in ((0, [plane * 8 + lax.rem(line + by, 8) for by in range(1, 8)]), (1, [lax.rem(plane + by, 16) * 8 + line for by in range(1, 16)])):
        hops = [copy(norms.at[turn, 0], norms.at[turn, by], n_s.at[turn, by], n_r.at[turn, by], to) for by, to in enumerate(others, 1)]
        for hop in hops:
            hop.start()
        for hop in hops:
            hop.wait()
        squares = jnp.sum(norms[turn, 0 : len(hops) + 1], axis=0)
        if turn == 0:
            norms[1, 0] = squares
    squares = jnp.sum(squares, axis=1, keepdims=True)
    factor = jnp.minimum(1.0, 0.5 * lax.rsqrt(squares / count + 1e-30))

    def adamw(w, m, v, g):
        g = g * factor
        m = 0.9 * m + 0.1 * g
        v = 0.95 * v + 0.05 * g * g
        step = m * lax.rsqrt(v + 1e-8) + 0.1 * w
        return (w - 0.02 * step).astype(BF16), m, v

    for one in own:
        one.wait()
    for n in EACH:
        copy(quad_g.at[q], quad_g.at[q], x_s.at[n], x_r.at[n], quad[n]).wait_send()
        theirs = quad_g.at[lax.rem(q + n + 1, 4)]
        copy(theirs, theirs, x_s.at[2 - n], x_r.at[2 - n], quad[n]).wait_recv()
    n_rows = md.shape[0]
    for l in SIDES:
        for n in PLACES:
            rows[0, :, n * quarter : (n + 1) * quarter] = f32(quad_g[n, l]).reshape(4 * n_rows, quarter)
        rows[1] = f32(own_d[l]).reshape(4 * n_rows, 4 * quarter)
        for n in PLACES:

            @pl.when(q == n)
            def _():
                mine = slice(n * n_rows, (n + 1) * n_rows)
                new, m, v = adamw(rows[1, mine, :], md2[:, l, :], vd2[:, l, :], rows[0, mine, :])
                new_rows[l] = new
                md2[:, l, :] = m
                vd2[:, l, :] = v
                cols[n, l] = new[:, n * quarter : (n + 1) * quarter]

    def piece(n):
        to = lax.rem(q + n + 1, 4)
        return new_rows.at[:, :, pl.ds(pl.multiple_of(to * quarter, quarter), quarter)]

    for n in EACH:
        copy(piece(n), cols.at[q], x_s.at[3 + n], x_r.at[3 + n], quad[n]).start()

    for i, own_w, m_ref, v_ref in ((0, own_g, mg2, vg2), (1, own_u, mu2, vu2)):
        for l in SIDES:
            new, m_ref[l], v_ref[l] = adamw(f32(own_w[l]), m_ref[l], v_ref[l], f32(P2[i][0, l]))
            at(i, l, *home[i], k)[...] = new

    def back_c(i, kind):
        d = kind % 2
        a, b, c = home[i]
        if kind < 2:
            ref = at(i, ALL, a, b, c, k)
        else:
            ref = at(i, d, a, b, rel(i, C, BEHIND[d]), k)
        return copy(ref, ref, c_s.at[i, kind], c_r.at[i, kind], near(AXES[i][2], AHEAD[d]))

    def came_c(i, kind):
        d = kind % 2
        a, b, _ = home[i]
        ref = at(i, ALL, a, b, rel(i, C, BEHIND[d]), k) if kind < 2 else at(i, d, a, b, rel(i, C, FAR), k)
        copy(ref, ref, c_s.at[i, kind], c_r.at[i, kind], partner).wait_recv()

    def back_b(i, kind):
        d = kind % 2
        a, b, _ = home[i]
        if kind < 2:
            ref = at(i, ALL, a, b, ALL, k)
        else:
            ref = at(i, d, a, rel(i, B, BEHIND[d]), ALL, k)
        return copy(ref, ref, b_s.at[i, kind, 0], b_r.at[i, kind, 0], near(AXES[i][1], AHEAD[d]))

    def came_b(i, kind):
        d = kind % 2
        ref = at(i, ALL, home[i][0], rel(i, B, BEHIND[d]), ALL, k) if kind < 2 else at(i, d, home[i][0], rel(i, B, FAR), ALL, k)
        copy(ref, ref, b_s.at[i, kind, 0], b_r.at[i, kind, 0], partner).wait_recv()

    def back_a(i, kind, rb):
        d, b = kind % 2, rel(i, B, rb)
        if kind < 2:
            ref = at(i, ALL, home[i][0], b, ALL, k)
        else:
            ref = at(i, d, rel(i, A, BEHIND[d]), b, ALL, k)
        return copy(ref, ref, a_s.at[i, kind, rb], a_r.at[i, kind, rb], near(AXES[i][0], AHEAD[d]))

    def came_a(i, kind, rb):
        d, b = kind % 2, rel(i, B, rb)
        ref = at(i, ALL, rel(i, A, BEHIND[d]), b, ALL, k) if kind < 2 else at(i, d, rel(i, A, FAR), b, ALL, k)
        copy(ref, ref, a_s.at[i, kind, rb], a_r.at[i, kind, rb], partner).wait_recv()

    def share(i, ra, rb):
        ref = at(i, ALL, rel(i, A, ra), rel(i, B, rb), ALL, k)
        return copy(ref, ref, d2d_s.at[i, ra, rb], d2d_r.at[i, ra, rb], partner)

    def shared(i, ra, rb):
        ref = at(i, ALL, rel(i, A, ra), rel(i, B, rb), ALL, 1 - k)
        copy(ref, ref, d2d_s.at[i, ra, rb], d2d_r.at[i, ra, rb], partner).wait_recv()

    def spread(i, c):
        a, b, _ = home[i]
        ref = at(i, ALL, a, b, c, k)
        for d in SIDES:
            copy(ref, ref, b_s.at[i, d, 0], b_r.at[i, d, 0], near(AXES[i][1], AHEAD[d])).start()
        for d in SIDES:
            copy(ref, ref, a_s.at[i, d, 0], a_r.at[i, d, 0], near(AXES[i][0], AHEAD[d])).start()

    def begin(i):
        for kind in SIDES:
            back_c(i, kind).start()
        spread(i, home[i][2])

    begin(0)
    begin(1)
    for n in EACH:
        copy(piece(n), cols.at[q], x_s.at[3 + n], x_r.at[3 + n], quad[n]).wait_send()
        theirs = cols.at[lax.rem(q + n + 1, 4)]
        copy(theirs, theirs, x_s.at[5 - n], x_r.at[5 - n], quad[n]).wait_recv()
    for l in SIDES:
        for n in PLACES:
            rows[0, n * n_rows : (n + 1) * n_rows, 0:quarter] = f32(cols[n, l])
        at(2, l, *home[2], k)[...] = rows[0, :, 0:quarter].reshape(n_rows // 2, 8, quarter).astype(BF16)
    begin(2)
    for i in EACH:
        for d in SIDES:
            came_c(i, d)
            back_c(i, 2 + d).start()
        for d in SIDES:
            spread(i, rel(i, C, AHEAD[d]))
    for i in EACH:
        for d in SIDES:
            came_c(i, 2 + d)
        spread(i, rel(i, C, FAR))
        share(i, 0, 0).start()
    for i in EACH:
        for d in SIDES:
            came_b(i, d)
            back_b(i, 2 + d).start()
    for i in EACH:
        for rb in (3, 1):
            for kind in SIDES:
                back_a(i, kind, rb).start()
            share(i, 0, rb).start()
    for i in EACH:
        for d in SIDES:
            came_b(i, 2 + d)
        for kind in SIDES:
            back_a(i, kind, 2).start()
        share(i, 0, 2).start()

    def pass_on(j):
        rb = lax.rem(order(j) + 2, 4)
        for i in EACH:
            for d in SIDES:
                came_a(i, d, rb)
                back_a(i, 2 + d, rb).start()
                share(i, BEHIND[d], rb).start()

    loop(pass_on, 3)

    def tail(i, d, c):
        ref = at(i, d, rel(i, A, BEHIND[d]), rel(i, B, FAR), c, k)
        return copy(ref, ref, a_s.at[i, 2 + d, 2], tail_r.at[i, d, c], near(AXES[i][0], AHEAD[d]))

    for i in EACH:
        for d in SIDES:
            came_a(i, d, 2)

    def pass_tail(c):
        for i in EACH:
            for d in SIDES:
                tail(i, d, c).start()

    loop(pass_tail)
    for i in EACH:
        for d in SIDES:
            share(i, BEHIND[d], 2).start()

    def last(j):
        rb = lax.rem(order(j) + 2, 4)
        for i in EACH:
            for d in SIDES:
                came_a(i, 2 + d, rb)
            share(i, 2, rb).start()

    loop(last, 3)

    def last_tail(c):
        for i in EACH:
            for d in SIDES:
                ref = at(i, d, rel(i, A, FAR), rel(i, B, FAR), c, k)
                copy(ref, ref, a_s.at[i, 2 + d, 2], tail_r.at[i, d, c], partner).wait_recv()
            ref = at(i, ALL, rel(i, A, FAR), rel(i, B, FAR), c, k)
            copy(ref, ref, d2d_s.at[i, 2, 2], d2d_r.at[i, 2, 2], partner).start()

    loop(last_tail)

    def finish(j):
        for i in EACH:
            for ra in PLACES:
                shared(i, ra, j)
                share(i, ra, j).wait_send()
            for kind in PLACES:
                back_a(i, kind, j).wait_send()

    loop(finish)
    for i in EACH:
        for kind in PLACES:
            back_b(i, kind).wait_send()
            back_c(i, kind).wait_send()


def write_wide(n_wide, *refs):
    sems = refs[-1]
    copies = [
        pltpu.make_async_copy(W.at[l, n], out.at[l, n], sems.at[8 * i + 4 * l + n]) for i, (W, out) in enumerate(zip(refs[:n_wide], refs[n_wide:-1])) for l in SIDES for n in PLACES
    ]
    for one in copies:
        one.start()
    for one in copies:
        one.wait()


def write_tall(n_small, W, *refs):
    small_in, out, small_out, sems = refs[:n_small], refs[n_small], refs[n_small + 1 : -1], refs[-1]
    quarter = W.shape[-1]
    copies = [pltpu.make_async_copy(r, o, sems.at[n]) for n, (r, o) in enumerate(zip(small_in, small_out))]
    for n in PLACES:
        for half in SIDES:
            columns = slice(n * quarter, (n + 1) * quarter)
            copies.append(pltpu.make_async_copy(W.at[:, :, :, 2 * half + n // 2, n % 2], out.at[:, :, :, half, :, :, columns], sems.at[len(copies)]))
    for one in copies:
        one.start()
    for one in copies:
        one.wait()


def solution(mesh):
    def step(*arrays):
        terms, weights, m, v = (arrays[i : i + 3] for i in (0, 3, 6, 9))
        wide, tall = weights[0].shape[2], weights[2].shape[2]
        n_rows = m[2].shape[1]
        m, v = ([jnp.swapaxes(one, 0, 1) if n == 2 else one for n, one in enumerate(some)] for some in (m, v))
        whole = (LAYERS, 4, 4, 4, 2, 8, wide)
        whole_d = (LAYERS, 4, 4, 2, n_rows // 2, 8, tall)
        shapes = (whole, whole, whole_d)
        quarter = tall // 4
        units = ((8, wide), (8, wide), (n_rows // 2, 8, quarter))
        g = [t[0].reshape(s) for t, s in zip(terms, shapes)]
        w = [t.reshape(s) for t, s in zip(weights, shapes)]
        count = float(sum(one.size for one in weights))
        blocks = [pltpu.VMEM((LAYERS, 4, 4, 4, 2, *u), BF16) for u in units]
        moments = [pltpu.VMEM(one.shape, F32) for one in (*m, *v)]
        hbm, vmem = pl.BlockSpec(memory_space=pltpu.HBM), pl.BlockSpec(memory_space=pltpu.VMEM)
        dma = pltpu.SemaphoreType.DMA
        results = pl.pallas_call(
            functools.partial(step_kernel, count),
            out_shape=blocks + moments,
            in_specs=[hbm] * 12,
            out_specs=[vmem] * 9,
            scratch_shapes=[
                *[pltpu.VMEM((2, 4, 4, *u), BF16) for u in units],
                *[pltpu.VMEM((2, LAYERS, 4, 4, *u), BF16) for u in units],
                *[pltpu.VMEM((2, 4, *u), BF16) for u in units],
                *[pltpu.VMEM((2, LAYERS, 4, *u), BF16) for u in units],
                *[pltpu.VMEM((2, *u), BF16) for u in units],
                *[pltpu.VMEM((2, LAYERS, *u), BF16) for u in units],
                pltpu.VMEM((LAYERS, 8, wide), BF16),
                pltpu.VMEM((LAYERS, 8, wide), BF16),
                pltpu.VMEM((LAYERS, n_rows // 2, 8, tall), BF16),
                pltpu.VMEM((4, LAYERS, *units[2]), BF16),
                pltpu.VMEM((2, 4 * n_rows, tall), F32),
                pltpu.VMEM((LAYERS, n_rows, tall), BF16),
                pltpu.VMEM((4, LAYERS, n_rows, quarter), BF16),
                pltpu.VMEM((2, 16, 1, 128), F32),
                dma((3, 4, 4)), dma((9,)), dma((3, 4, 4)), dma((3, 4, 4)),
                dma((3, 6, 4)), dma((3, 6, 4)), dma((3, 6, 4)), dma((3, 6, 4)), dma((3, 6)), dma((3, 6)),
                dma((6,)), dma((6,)), dma((2, 16)), dma((2, 16)), dma((3, 4)), dma((3, 4)), dma((3, 2, 4)),
            ],
            compiler_params=pltpu.CompilerParams(collective_id=0, has_side_effects=True, vmem_limit_bytes=26600000),
            name="step",
        )(*g, *w, *m, *v)

        def write(kernel, arrays, outs):
            return pl.pallas_call(
                kernel,
                out_shape=outs,
                in_specs=[vmem] * len(arrays),
                out_specs=[hbm] * len(outs),
                scratch_shapes=[dma((16,))],
                compiler_params=pltpu.CompilerParams(vmem_limit_bytes=2**20),
                name="write",
            )(*arrays)

        outs = [jax.ShapeDtypeStruct(s, BF16) for s in shapes]
        small = results[3:]
        new_gate, new_up = write(functools.partial(write_wide, 2), results[:2], outs[:2])
        new_down, *moved = write(functools.partial(write_tall, len(small)), results[2:], outs[2:] + [jax.ShapeDtypeStruct(one.shape, F32) for one in small])
        new = [r.reshape(t.shape) for r, t in zip((new_gate, new_up, new_down), weights)]
        return (*new, *(jnp.swapaxes(one, 0, 1) if n % 3 == 2 else one for n, one in enumerate(moved)))

    all_of, cut = P(None, None, None), P(None, "dp", None)
    return jax.shard_map(
        step,
        mesh=mesh,
        in_specs=(P(("rep", "dp"), None, None, None),) * 3 + (all_of,) * 3 + (cut,) * 6,
        out_specs=(P("rep", None, None),) * 3 + (P("rep", "dp", None),) * 6,
        check_vma=False,
    )
```

```python
import functools

import jax
import jax.numpy as jnp
from jax import lax
from jax.experimental import pallas as pl
from jax.experimental.pallas import tpu as pltpu
from jax.sharding import PartitionSpec as P

MESH = pl.DeviceIdType.MESH
F32, BF16 = jnp.float32, jnp.bfloat16
AXES = ((0, 1, 2), (1, 2, 0), (2, 0, 1))
LAYERS = 2
A, B, C = range(3)
FAR = 2
EACH, SIDES, PLACES, OTHERS, LANDED = range(3), range(2), range(4), range(1, 4), range(2, 6)
AHEAD, BEHIND = (1, 3), (3, 1)


def order(j):
    return lax.rem(2 + j + lax.div(j, 2) * (2 * j - 3), 4)


def loop(body, n=4, start=0):
    lax.fori_loop(start, n, lambda j, c: (body(j), c)[1], 0)


def f32(x):
    return x.astype(F32)


def step_kernel(
    count, gg, gu, gd, wg, wu, wd, mg, mu, md, vg, vu, vd,
    Wg, Wu, Wd, mg2, mu2, md2, vg2, vu2, vd2,
    R1g, R1u, R1d, R2g, R2u, R2d, Q1g, Q1u, Q1d, Q2g, Q2u, Q2d, P1g, P1u, P1d, P2g, P2u, P2d,
    own_g, own_u, own_d, quad_g, rows, new_rows, cols, norms,
    load_sem, own_sem, d2d_s, d2d_r, a_s, a_r, b_s, b_r, c_s, c_r, x_s, x_r, n_s, n_r, piece_l, piece_r, tail_r, share_r,
):
    g_in, W, w_in = (gg, gu, gd), (Wg, Wu, Wd), (wg, wu, wd)
    R1, R2, Q1, Q2, P1, P2 = (R1g, R1u, R1d), (R2g, R2u, R2d), (Q1g, Q1u, Q1d), (Q2g, Q2u, Q2d), (P1g, P1u, P1d), (P2g, P2u, P2d)
    quarter = cols.shape[-1]
    me = lax.axis_index("dp")
    k = lax.rem(me, 2)
    pos = (me // 32, lax.rem(me // 8, 4), lax.rem(me // 2, 4))
    q = lax.rem(me, 4)

    def device(p, core):
        return ((p[0] * 4 + p[1]) * 4 + p[2]) * 2 + core

    def near(axis, by):
        return device([lax.rem(c + by, 4) if n == axis else c for n, c in enumerate(pos)], k)

    partner = device(pos, 1 - k)
    quad = [me - q + lax.rem(q + by, 4) for by in OTHERS]

    def copy(src, dst, send, recv, to):
        return pltpu.make_async_remote_copy(src_ref=src, dst_ref=dst, send_sem=send, recv_sem=recv, device_id={"dp": to}, device_id_type=MESH)

    def at(i, l, a, b, c, core):
        place = dict(zip(AXES[i], (a, b, c)))
        return W[i].at[l, place[0], place[1], place[2], core]

    ALL = slice(None)
    home = [[pos[n] for n in AXES[i]] for i in EACH]

    around = [[lax.rem(one + by, 4) for by in PLACES] for one in pos]

    def rel(i, which, by):
        if isinstance(by, int):
            return around[AXES[i][which]][by]
        return lax.rem(home[i][which] + by, 4)

    def sent(ref, sem):
        copy(ref, ref, sem, x_r.at[0], partner).wait_send()

    def landed(ref, sem):
        copy(ref, ref, x_s.at[0], sem, partner).wait_recv()

    def source(i, a, b, c, core):
        if i == 0:
            return gg.at[:, a, b, c, core]
        if i == 1:
            return gu.at[:, c, a, b, core]
        columns = pl.ds(pl.multiple_of(lax.rem(a, 2) * (2 * quarter) + core * quarter, quarter), quarter)
        return gd.at[:, b, c, a // 2, :, :, columns]

    def load(i, ra, rb):
        a, b = rel(i, A, ra), rel(i, B, rb)
        return pltpu.make_async_copy(source(i, a, b, ALL, k), at(i, ALL, a, b, ALL, k), load_sem.at[i, ra, rb])

    def trade(i, ra, rb):
        a, b = rel(i, A, ra), rel(i, B, rb)
        return copy(source(i, a, b, ALL, 1 - k), at(i, ALL, a, b, ALL, k), d2d_s.at[i], d2d_r.at[i, ra, rb], partner)

    def first_load(i, c):
        a, b = rel(i, A, FAR), rel(i, B, FAR)
        return pltpu.make_async_copy(source(i, a, b, c, k), at(i, ALL, a, b, c, k), piece_l.at[i, c])

    def first_trade(i, c):
        a, b = rel(i, A, FAR), rel(i, B, FAR)
        return copy(source(i, a, b, c, 1 - k), at(i, ALL, a, b, c, k), d2d_s.at[i], piece_r.at[i, c], partner)

    def first_traded(i, c):
        a, b = rel(i, A, FAR), rel(i, B, FAR)
        first_load(i, c).wait()
        ref = at(i, ALL, a, b, c, 1 - k)
        copy(ref, ref, d2d_s.at[i], piece_r.at[i, c], partner).wait_recv()

    def traded(i, ra, rb):
        a, b = rel(i, A, ra), rel(i, B, rb)
        load(i, ra, rb).wait()
        copy(at(i, ALL, a, b, ALL, 1 - k), at(i, ALL, a, b, ALL, 1 - k), d2d_s.at[i], d2d_r.at[i, ra, rb], partner).wait_recv()

    across = me - q + (2 - 2 * (q // 2)) + (1 - k)
    peers = [partner, across] + [near(axis, by) for axis in EACH for by in AHEAD]
    barrier = pltpu.get_barrier_semaphore()
    for peer in peers:
        pl.semaphore_signal(barrier, inc=1, device_id={"dp": peer}, device_id_type=MESH)

    def start_all(what, ras, start=0):
        def body(j):
            for ra in ras:
                for i in EACH:
                    what(i, ra, order(j)).start()

        loop(body, start=start)

    def start_first(what):
        def body(c):
            for i in EACH:
                what(i, c).start()

        loop(body)

    start_first(first_load)
    start_all(load, (2,), 1)
    pl.semaphore_wait(barrier, len(peers))
    start_first(first_trade)
    start_all(trade, (2,), 1)
    for ras in (AHEAD, (0,)):
        start_all(load, ras)
        start_all(trade, ras)
    own = [
        pltpu.make_async_copy(wg.at[:, pos[0], pos[1], pos[2], k], own_g, own_sem.at[0]),
        pltpu.make_async_copy(wu.at[:, pos[0], pos[1], pos[2], k], own_u, own_sem.at[1]),
        pltpu.make_async_copy(wd.at[:, pos[0], pos[1], pos[2] // 2], own_d, own_sem.at[2]),
    ]
    for n, (moment, there) in enumerate(zip((mg, mu, md, vg, vu, vd), (mg2, mu2, md2, vg2, vu2, vd2))):
        own.append(pltpu.make_async_copy(moment, there, own_sem.at[3 + n]))
    for one in own:
        one.start()

    def sum0(i, l, a, b, c):
        return f32(at(i, l, a, b, c, k)[...]) + f32(at(i, l, a, b, c, 1 - k)[...])

    def sum1(i, l, b, c):
        return sum0(i, l, home[i][0], b, c) + f32(R2[i][0, l, b, c]) + f32(R2[i][1, l, b, c])

    def sum2(i, l, c):
        return sum1(i, l, home[i][1], c) + f32(Q2[i][0, l, c]) + f32(Q2[i][1, l, c])

    def sum3(i, l):
        return sum2(i, l, home[i][2]) + f32(P2[i][0, l]) + f32(P2[i][1, l])

    def hop_a(i, kind, rb):
        d, b = kind % 2, rel(i, B, rb)
        to = near(AXES[i][0], AHEAD[d])
        if kind < 2:
            src, dst = at(i, d, rel(i, A, FAR), b, ALL, k), R1[i].at[d, b]
        elif kind < 4:
            src, dst = at(i, 1 - d, rel(i, A, AHEAD[d]), b, ALL, k), R2[i].at[d, 1 - d, b]
        else:
            src, dst = R1[i].at[d, b], R2[i].at[d, d, b]
        return copy(src, dst, a_s.at[i, min(kind // 2, 1)], a_r.at[i, min(kind, 2), rb], to)

    def hop_b(i, kind, rc):
        d, c = kind % 2, rel(i, C, rc)
        to = near(AXES[i][1], AHEAD[d])
        if kind < 2:
            src, dst = R2[i].at[0, d, rel(i, B, FAR), c], Q1[i].at[d, c]
        elif kind < 4:
            src, dst = R2[i].at[0, 1 - d, rel(i, B, AHEAD[d]), c], Q2[i].at[d, 1 - d, c]
        else:
            src, dst = Q1[i].at[d, c], Q2[i].at[d, d, c]
        return copy(src, dst, b_s.at[i, min(kind // 2, 1)], b_r.at[i, min(kind, 2), rc], to)

    def hop_c(i, kind):
        d = kind % 2
        to = near(AXES[i][2], AHEAD[d])
        if kind < 2:
            src, dst = Q2[i].at[0, d, rel(i, C, FAR)], P1[i].at[d]
        elif kind < 4:
            src, dst = Q2[i].at[0, 1 - d, rel(i, C, AHEAD[d])], P2[i].at[d, 1 - d]
        else:
            src, dst = P1[i].at[d], P2[i].at[d, d]
        return copy(src, dst, c_s.at[i, min(kind // 2, 1)], c_r.at[i, min(kind, 2)], to)

    def farthest(j):
        rb = order(j)
        for i in EACH:
            traded(i, 2, rb)
            a, b = rel(i, A, FAR), rel(i, B, rb)

            def add(t):
                at(i, t // 4, a, b, lax.rem(t, 4), k)[...] = sum0(i, t // 4, a, b, lax.rem(t, 4)).astype(BF16)

            loop(add, 8)
            hop_a(i, 0, rb).start()
            hop_a(i, 1, rb).start()

    def farthest_first(c):
        for i in EACH:
            first_traded(i, c)
            a, b = rel(i, A, FAR), rel(i, B, FAR)
            for l in SIDES:
                ref = at(i, l, a, b, c, k)
                ref[...] = sum0(i, l, a, b, c).astype(BF16)
                copy(ref, R1[i].at[l, b, c], a_s.at[i, 0], a_r.at[i, l, 2], near(AXES[i][0], AHEAD[l])).start()

    loop(farthest_first)
    loop(farthest, start=1)

    def plain(j):
        rb = order(j)
        for i in EACH:
            for d in SIDES:
                ra = AHEAD[d]
                traded(i, ra, rb)
                a, b = rel(i, A, ra), rel(i, B, rb)

                def add(c):
                    at(i, 1 - d, a, b, c, k)[...] = sum0(i, 1 - d, a, b, c).astype(BF16)

                loop(add)
                hop_a(i, 2 + d, rb).start()

    loop(plain)

    def onward(j):
        rb = order(j)
        for i in EACH:
            for d in SIDES:
                hop_a(i, d, rb).wait_recv()
                a, b = rel(i, A, AHEAD[d]), rel(i, B, rb)

                def add(c):
                    R1[i][d, b, c] = (f32(R1[i][d, b, c]) + sum0(i, d, a, b, c)).astype(BF16)

                loop(add)
                hop_a(i, 4 + d, rb).start()

    loop(onward)

    def arrived_a(i, rb):
        traded(i, 0, rb)
        landed(R1[i].at[0], a_r.at[i, 2, rb])

    def settle_a(i, l, rb, rc):
        b, c = rel(i, B, rb), rel(i, C, rc)
        R2[i][0, l, b, c] = sum1(i, l, b, c).astype(BF16)

    for i in EACH:
        arrived_a(i, 2)

        def far_b(j, i=i):
            for d in SIDES:
                settle_a(i, d, 2, order(j))
                hop_b(i, d, order(j)).start()

        loop(far_b)
    for rb in AHEAD:
        for i in EACH:
            arrived_a(i, rb)

    def near_b(j):
        rc = order(j)
        for i in EACH:
            for d in SIDES:
                settle_a(i, 1 - d, AHEAD[d], rc)
                hop_b(i, 2 + d, rc).start()
        for i in EACH:
            for d in SIDES:
                hop_b(i, d, rc).wait_recv()
                c = rel(i, C, rc)
                Q1[i][d, c] = (f32(Q1[i][d, c]) + sum1(i, d, rel(i, B, AHEAD[d]), c)).astype(BF16)
                hop_b(i, 4 + d, rc).start()

    loop(near_b)
    for i in EACH:
        sent(R1[i], a_s.at[i, 0])
        sent(R2[i], a_s.at[i, 1])
        sent(at(i, ALL, ALL, ALL, ALL, k), d2d_s.at[i])
    for i in EACH:
        arrived_a(i, 0)

    def arrived_b(i, rc):
        landed(P2[i], b_r.at[i, 2, rc])

    for i in EACH:
        arrived_b(i, 2)
        for d in SIDES:
            c = rel(i, C, FAR)
            Q2[i][0, d, c] = sum2(i, d, c).astype(BF16)
            hop_c(i, d).start()
    for d in (1, 0):
        for i in EACH:
            arrived_b(i, AHEAD[d])
            c = rel(i, C, AHEAD[d])
            Q2[i][0, 1 - d, c] = sum2(i, 1 - d, c).astype(BF16)
            hop_c(i, 2 + d).start()
    for i in EACH:
        sent(Q1[i], b_s.at[i, 0])
        sent(Q2[i], b_s.at[i, 1])
    for i in EACH:
        for d in SIDES:
            hop_c(i, d).wait_recv()
            P1[i][d] = (f32(P1[i][d]) + sum2(i, d, rel(i, C, AHEAD[d]))).astype(BF16)
            hop_c(i, 4 + d).start()
    for i in EACH:
        arrived_b(i, 0)
    squares = jnp.zeros((8, 128), F32)
    for i in (2, 0, 1):
        landed(P2[i], c_r.at[i, 2])
        for l in SIDES:
            total = sum3(i, l).astype(BF16)
            if i == 2:
                quad_g[q, l] = total
            else:
                P2[i][0, l] = total
            s = f32(total)
            s = s * s
            if i == 2:
                s = jnp.sum(s, axis=0)
            for lane in range(0, s.shape[-1], 128):
                squares = squares + s[:, lane : lane + 128]
        if i == 2:
            for n in EACH:
                copy(quad_g.at[q], quad_g.at[q], x_s.at[n], x_r.at[n], quad[n]).start()
    norms[0, 0] = jnp.sum(squares, axis=0, keepdims=True)

    for i in EACH:
        sent(P1[i], c_s.at[i, 0])
        sent(P2[i], c_s.at[i, 1])

    line, plane = lax.rem(me, 8), me // 8
    for turn, others in ((0, [plane * 8 + lax.rem(line + by, 8) for by in range(1, 8)]), (1, [lax.rem(plane + by, 16) * 8 + line for by in range(1, 16)])):
        hops = [copy(norms.at[turn, 0], norms.at[turn, by], n_s.at[turn, by], n_r.at[turn, by], to) for by, to in enumerate(others, 1)]
        for hop in hops:
            hop.start()
        for hop in hops:
            hop.wait()
        squares = jnp.sum(norms[turn, 0 : len(hops) + 1], axis=0)
        if turn == 0:
            norms[1, 0] = squares
    squares = jnp.sum(squares, axis=1, keepdims=True)
    factor = jnp.minimum(1.0, 0.5 * lax.rsqrt(squares / count + 1e-30))

    def adamw(w, m, v, g):
        g = g * factor
        m = 0.9 * m + 0.1 * g
        v = 0.95 * v + 0.05 * g * g
        step = m * lax.rsqrt(v + 1e-8) + 0.1 * w
        return (w - 0.02 * step).astype(BF16), m, v

    for one in own:
        one.wait()
    for n in EACH:
        copy(quad_g.at[q], quad_g.at[q], x_s.at[n], x_r.at[n], quad[n]).wait_send()
        theirs = quad_g.at[lax.rem(q + n + 1, 4)]
        copy(theirs, theirs, x_s.at[2 - n], x_r.at[2 - n], quad[n]).wait_recv()
    n_rows = md.shape[0]
    for l in SIDES:
        for n in PLACES:
            rows[0, :, n * quarter : (n + 1) * quarter] = f32(quad_g[n, l]).reshape(4 * n_rows, quarter)
        rows[1] = f32(own_d[l]).reshape(4 * n_rows, 4 * quarter)
        for n in PLACES:

            @pl.when(q == n)
            def _():
                mine = slice(n * n_rows, (n + 1) * n_rows)
                new, m, v = adamw(rows[1, mine, :], md2[:, l, :], vd2[:, l, :], rows[0, mine, :])
                new_rows[l] = new
                md2[:, l, :] = m
                vd2[:, l, :] = v
                cols[n, l] = new[:, n * quarter : (n + 1) * quarter]

    def piece(n):
        to = lax.rem(q + n + 1, 4)
        return new_rows.at[:, :, pl.ds(pl.multiple_of(to * quarter, quarter), quarter)]

    for n in EACH:
        copy(piece(n), cols.at[q], x_s.at[3 + n], x_r.at[3 + n], quad[n]).start()

    for i, own_w, m_ref, v_ref in ((0, own_g, mg2, vg2), (1, own_u, mu2, vu2)):
        for l in SIDES:
            new, m_ref[l], v_ref[l] = adamw(f32(own_w[l]), m_ref[l], v_ref[l], f32(P2[i][0, l]))
            at(i, l, *home[i], k)[...] = new

    def back_c(i, kind):
        d = kind % 2
        a, b, c = home[i]
        if kind < 2:
            ref = at(i, ALL, a, b, c, k)
        else:
            ref = at(i, d, a, b, rel(i, C, BEHIND[d]), k)
        return copy(ref, ref, c_s.at[i, 1 - kind // 2], c_r.at[i, min(kind, 2)], near(AXES[i][2], AHEAD[d]))

    def came_c(i, d):
        a, b, _ = home[i]
        landed(at(i, ALL, a, b, rel(i, C, BEHIND[d]), k), c_r.at[i, d])

    def back_b(i, kind):
        d = kind % 2
        a, b, _ = home[i]
        if kind < 2:
            ref = at(i, ALL, a, b, ALL, k)
        else:
            ref = at(i, d, a, rel(i, B, BEHIND[d]), ALL, k)
        return copy(ref, ref, b_s.at[i, 1 - kind // 2], b_r.at[i, min(kind, 2), 0], near(AXES[i][1], AHEAD[d]))

    def came_b(i, d):
        landed(at(i, ALL, home[i][0], rel(i, B, BEHIND[d]), ALL, k), b_r.at[i, d, 0])

    def back_a(i, kind, rb):
        d, b = kind % 2, rel(i, B, rb)
        if kind < 2:
            ref = at(i, ALL, home[i][0], b, ALL, k)
        else:
            ref = at(i, d, rel(i, A, BEHIND[d]), b, ALL, k)
        return copy(ref, ref, a_s.at[i, 1 - kind // 2], a_r.at[i, min(kind, 2), rb], near(AXES[i][0], AHEAD[d]))

    def came_a(i, d, rb):
        landed(at(i, ALL, rel(i, A, BEHIND[d]), rel(i, B, rb), ALL, k), a_r.at[i, d, rb])

    def share(i, ra, rb):
        ref = at(i, ALL, rel(i, A, ra), rel(i, B, rb), ALL, k)
        return copy(ref, ref, d2d_s.at[i], share_r.at[i], partner)

    def spread(i, c):
        a, b, _ = home[i]
        ref = at(i, ALL, a, b, c, k)
        for d in SIDES:
            copy(ref, ref, b_s.at[i, 1], b_r.at[i, d, 0], near(AXES[i][1], AHEAD[d])).start()
        for d in SIDES:
            copy(ref, ref, a_s.at[i, 1], a_r.at[i, d, 0], near(AXES[i][0], AHEAD[d])).start()

    def begin(i):
        for kind in SIDES:
            back_c(i, kind).start()
        spread(i, home[i][2])

    begin(0)
    begin(1)
    for n in EACH:
        copy(piece(n), cols.at[q], x_s.at[3 + n], x_r.at[3 + n], quad[n]).wait_send()
        theirs = cols.at[lax.rem(q + n + 1, 4)]
        copy(theirs, theirs, x_s.at[5 - n], x_r.at[5 - n], quad[n]).wait_recv()
    for l in SIDES:
        for n in PLACES:
            rows[0, n * n_rows : (n + 1) * n_rows, 0:quarter] = f32(cols[n, l])
        at(2, l, *home[2], k)[...] = rows[0, :, 0:quarter].reshape(n_rows // 2, 8, quarter).astype(BF16)
    begin(2)
    for i in EACH:
        for d in SIDES:
            came_c(i, d)
            back_c(i, 2 + d).start()
        for d in SIDES:
            spread(i, rel(i, C, AHEAD[d]))
    for i in EACH:
        landed(P1[i], c_r.at[i, 2])
        spread(i, rel(i, C, FAR))
        share(i, 0, 0).start()
    for i in EACH:
        for d in SIDES:
            came_b(i, d)
            back_b(i, 2 + d).start()
    for i in EACH:
        for rb in (3, 1):
            for kind in SIDES:
                back_a(i, kind, rb).start()
            share(i, 0, rb).start()
    for i in EACH:
        landed(Q1[i], b_r.at[i, 2, 0])
        for kind in SIDES:
            back_a(i, kind, 2).start()
        share(i, 0, 2).start()

    def pass_on(j):
        rb = lax.rem(order(j) + 2, 4)
        for i in EACH:
            for d in SIDES:
                came_a(i, d, rb)
                back_a(i, 2 + d, rb).start()
                share(i, BEHIND[d], rb).start()

    loop(pass_on, 3)

    def tail(i, d, c):
        ref = at(i, d, rel(i, A, BEHIND[d]), rel(i, B, FAR), c, k)
        return copy(ref, ref, a_s.at[i, 0], tail_r.at[i, c], near(AXES[i][0], AHEAD[d]))

    for i in EACH:
        for d in SIDES:
            came_a(i, d, 2)

    def pass_tail(c):
        for i in EACH:
            for d in SIDES:
                tail(i, d, c).start()

    loop(pass_tail)
    for i in EACH:
        for d in SIDES:
            share(i, BEHIND[d], 2).start()

    def last(j):
        rb = lax.rem(order(j) + 2, 4)
        for i in EACH:
            landed(Q1[i], a_r.at[i, 2, rb])
            share(i, 2, rb).start()

    loop(last, 3)

    def last_tail(c):
        for i in EACH:
            landed(P1[i], tail_r.at[i, c])
            ref = at(i, ALL, rel(i, A, FAR), rel(i, B, FAR), c, k)
            copy(ref, ref, d2d_s.at[i], share_r.at[i], partner).start()

    loop(last_tail)

    for i in EACH:
        sent(R1[i], a_s.at[i, 0])
        sent(R2[i], a_s.at[i, 1])
        sent(Q1[i], b_s.at[i, 0])
        sent(Q2[i], b_s.at[i, 1])
        sent(P1[i], c_s.at[i, 0])
        sent(P2[i], c_s.at[i, 1])
    for i in EACH:
        landed(at(i, ALL, ALL, ALL, ALL, 1 - k), share_r.at[i])
        sent(at(i, ALL, ALL, ALL, ALL, k), d2d_s.at[i])


def write_wide(n_wide, *refs):
    sems = refs[-1]
    copies = [
        pltpu.make_async_copy(W.at[l, n], out.at[l, n], sems.at[8 * i + 4 * l + n]) for i, (W, out) in enumerate(zip(refs[:n_wide], refs[n_wide:-1])) for l in SIDES for n in PLACES
    ]
    for one in copies:
        one.start()
    for one in copies:
        one.wait()


def write_tall(n_small, W, *refs):
    small_in, out, small_out, sems = refs[:n_small], refs[n_small], refs[n_small + 1 : -1], refs[-1]
    quarter = W.shape[-1]
    copies = [pltpu.make_async_copy(r, o, sems.at[n]) for n, (r, o) in enumerate(zip(small_in, small_out))]
    for n in PLACES:
        for half in SIDES:
            columns = slice(n * quarter, (n + 1) * quarter)
            copies.append(pltpu.make_async_copy(W.at[:, :, :, 2 * half + n // 2, n % 2], out.at[:, :, :, half, :, :, columns], sems.at[len(copies)]))
    for one in copies:
        one.start()
    for one in copies:
        one.wait()


def solution(mesh):
    def step(*arrays):
        terms, weights, m, v = (arrays[i : i + 3] for i in (0, 3, 6, 9))
        wide, tall = weights[0].shape[2], weights[2].shape[2]
        n_rows = m[2].shape[1]
        m, v = ([jnp.swapaxes(one, 0, 1) if n == 2 else one for n, one in enumerate(some)] for some in (m, v))
        whole = (LAYERS, 4, 4, 4, 2, 8, wide)
        whole_d = (LAYERS, 4, 4, 2, n_rows // 2, 8, tall)
        shapes = (whole, whole, whole_d)
        quarter = tall // 4
        units = ((8, wide), (8, wide), (n_rows // 2, 8, quarter))
        g = [t[0].reshape(s) for t, s in zip(terms, shapes)]
        w = [t.reshape(s) for t, s in zip(weights, shapes)]
        count = float(sum(one.size for one in weights))
        blocks = [pltpu.VMEM((LAYERS, 4, 4, 4, 2, *u), BF16) for u in units]
        moments = [pltpu.VMEM(one.shape, F32) for one in (*m, *v)]
        hbm, vmem = pl.BlockSpec(memory_space=pltpu.HBM), pl.BlockSpec(memory_space=pltpu.VMEM)
        dma = pltpu.SemaphoreType.DMA
        results = pl.pallas_call(
            functools.partial(step_kernel, count),
            out_shape=blocks + moments,
            in_specs=[hbm] * 12,
            out_specs=[vmem] * 9,
            scratch_shapes=[
                *[pltpu.VMEM((2, 4, 4, *u), BF16) for u in units],
                *[pltpu.VMEM((2, LAYERS, 4, 4, *u), BF16) for u in units],
                *[pltpu.VMEM((2, 4, *u), BF16) for u in units],
                *[pltpu.VMEM((2, LAYERS, 4, *u), BF16) for u in units],
                *[pltpu.VMEM((2, *u), BF16) for u in units],
                *[pltpu.VMEM((2, LAYERS, *u), BF16) for u in units],
                pltpu.VMEM((LAYERS, 8, wide), BF16),
                pltpu.VMEM((LAYERS, 8, wide), BF16),
                pltpu.VMEM((LAYERS, n_rows // 2, 8, tall), BF16),
                pltpu.VMEM((4, LAYERS, *units[2]), BF16),
                pltpu.VMEM((2, 4 * n_rows, tall), F32),
                pltpu.VMEM((LAYERS, n_rows, tall), BF16),
                pltpu.VMEM((4, LAYERS, n_rows, quarter), BF16),
                pltpu.VMEM((2, 16, 1, 128), F32),
                dma((3, 4, 4)), dma((9,)), dma((3,)), dma((3, 4, 4)),
                dma((3, 2)), dma((3, 3, 4)), dma((3, 2)), dma((3, 3, 4)), dma((3, 2)), dma((3, 3)),
                dma((6,)), dma((6,)), dma((2, 16)), dma((2, 16)), dma((3, 4)), dma((3, 4)), dma((3, 4)), dma((3,)),
            ],
            compiler_params=pltpu.CompilerParams(collective_id=0, has_side_effects=True, vmem_limit_bytes=26600000),
            name="step",
        )(*g, *w, *m, *v)

        def write(kernel, arrays, outs):
            return pl.pallas_call(
                kernel,
                out_shape=outs,
                in_specs=[vmem] * len(arrays),
                out_specs=[hbm] * len(outs),
                scratch_shapes=[dma((16,))],
                compiler_params=pltpu.CompilerParams(vmem_limit_bytes=2**20),
                name="write",
            )(*arrays)

        outs = [jax.ShapeDtypeStruct(s, BF16) for s in shapes]
        small = results[3:]
        new_gate, new_up = write(functools.partial(write_wide, 2), results[:2], outs[:2])
        new_down, *moved = write(functools.partial(write_tall, len(small)), results[2:], outs[2:] + [jax.ShapeDtypeStruct(one.shape, F32) for one in small])
        new = [r.reshape(t.shape) for r, t in zip((new_gate, new_up, new_down), weights)]
        return (*new, *(jnp.swapaxes(one, 0, 1) if n % 3 == 2 else one for n, one in enumerate(moved)))

    all_of, cut = P(None, None, None), P(None, "dp", None)
    return jax.shard_map(
        step,
        mesh=mesh,
        in_specs=(P(("rep", "dp"), None, None, None),) * 3 + (all_of,) * 3 + (cut,) * 6,
        out_specs=(P("rep", None, None),) * 3 + (P("rep", "dp", None),) * 6,
        check_vma=False,
    )
```

```python
import functools

import jax
import jax.numpy as jnp
from jax import lax
from jax.experimental import pallas as pl
from jax.experimental.pallas import tpu as pltpu
from jax.sharding import PartitionSpec as P

MESH = pl.DeviceIdType.MESH
F32, BF16 = jnp.float32, jnp.bfloat16
AXES = ((0, 1, 2), (1, 2, 0), (2, 0, 1))
LAYERS = 2
A, B, C = range(3)
FAR = 2
EACH, SIDES, PLACES, OTHERS, LANDED = range(3), range(2), range(4), range(1, 4), range(2, 6)
AHEAD, BEHIND = (1, 3), (3, 1)


def order(j):
    return lax.rem(2 + j + lax.div(j, 2) * (2 * j - 3), 4)


def loop(body, n=4, start=0):
    lax.fori_loop(start, n, lambda j, c: (body(j), c)[1], 0)


def f32(x):
    return x.astype(F32)


def step_kernel(
    count, gg, gu, gd, wg, wu, wd, mg, mu, md, vg, vu, vd,
    Wg, Wu, Wd, mg2, mu2, md2, vg2, vu2, vd2,
    R1g, R1u, R1d, R2g, R2u, R2d, Q1g, Q1u, Q1d, Q2g, Q2u, Q2d, P1g, P1u, P1d, P2g, P2u, P2d,
    partial_g, partial_u, partial_d, own_g, own_u, own_d, quad_g, rows, new_rows, cols, norms,
    load_sem, own_sem, d2d_s, d2d_r, a_s, a_r, b_s, b_r, c_s, c_r, x_s, x_r, n_s, n_r, piece_l, piece_r, tail_r, share_r,
):
    g_in, W, w_in = (gg, gu, gd), (Wg, Wu, Wd), (wg, wu, wd)
    R1, R2, Q1, Q2, P1, P2 = (R1g, R1u, R1d), (R2g, R2u, R2d), (Q1g, Q1u, Q1d), (Q2g, Q2u, Q2d), (P1g, P1u, P1d), (P2g, P2u, P2d)
    partial = (partial_g, partial_u, partial_d)
    quarter = cols.shape[-1]
    me = lax.axis_index("dp")
    k = lax.rem(me, 2)
    pos = (me // 32, lax.rem(me // 8, 4), lax.rem(me // 2, 4))
    q = lax.rem(me, 4)

    def device(p, core):
        return ((p[0] * 4 + p[1]) * 4 + p[2]) * 2 + core

    def near(axis, by):
        return device([lax.rem(c + by, 4) if n == axis else c for n, c in enumerate(pos)], k)

    partner = device(pos, 1 - k)
    quad = [me - q + lax.rem(q + by, 4) for by in OTHERS]

    def copy(src, dst, send, recv, to):
        return pltpu.make_async_remote_copy(src_ref=src, dst_ref=dst, send_sem=send, recv_sem=recv, device_id={"dp": to}, device_id_type=MESH)

    def at(i, l, a, b, c, core):
        place = dict(zip(AXES[i], (a, b, c)))
        return W[i].at[l, place[0], place[1], place[2], core]

    ALL = slice(None)
    home = [[pos[n] for n in AXES[i]] for i in EACH]

    around = [[lax.rem(one + by, 4) for by in PLACES] for one in pos]

    def rel(i, which, by):
        if isinstance(by, int):
            return around[AXES[i][which]][by]
        return lax.rem(home[i][which] + by, 4)

    def sent(ref, sem):
        copy(ref, ref, sem, x_r.at[0], partner).wait_send()

    def landed(ref, sem):
        copy(ref, ref, x_s.at[0], sem, partner).wait_recv()

    def source(i, a, b, c, core):
        if i == 0:
            return gg.at[:, a, b, c, core]
        if i == 1:
            return gu.at[:, c, a, b, core]
        columns = pl.ds(pl.multiple_of(lax.rem(a, 2) * (2 * quarter) + core * quarter, quarter), quarter)
        return gd.at[:, b, c, a // 2, :, :, columns]

    def load(i, ra, rb):
        a, b = rel(i, A, ra), rel(i, B, rb)
        return pltpu.make_async_copy(source(i, a, b, ALL, k), at(i, ALL, a, b, ALL, k), load_sem.at[i, ra, rb])

    def trade(i, ra, rb):
        a, b = rel(i, A, ra), rel(i, B, rb)
        return copy(source(i, a, b, ALL, 1 - k), at(i, ALL, a, b, ALL, k), d2d_s.at[i], d2d_r.at[i, ra, rb], partner)

    def first_load(i, c):
        a, b = rel(i, A, FAR), rel(i, B, FAR)
        return pltpu.make_async_copy(source(i, a, b, c, k), at(i, ALL, a, b, c, k), piece_l.at[i, c])

    def first_trade(i, c):
        a, b = rel(i, A, FAR), rel(i, B, FAR)
        return copy(source(i, a, b, c, 1 - k), at(i, ALL, a, b, c, k), d2d_s.at[i], piece_r.at[i, c], partner)

    def first_traded(i, c):
        a, b = rel(i, A, FAR), rel(i, B, FAR)
        first_load(i, c).wait()
        ref = at(i, ALL, a, b, c, 1 - k)
        copy(ref, ref, d2d_s.at[i], piece_r.at[i, c], partner).wait_recv()

    def traded(i, ra, rb):
        a, b = rel(i, A, ra), rel(i, B, rb)
        load(i, ra, rb).wait()
        copy(at(i, ALL, a, b, ALL, 1 - k), at(i, ALL, a, b, ALL, 1 - k), d2d_s.at[i], d2d_r.at[i, ra, rb], partner).wait_recv()

    across = me - q + (2 - 2 * (q // 2)) + (1 - k)
    peers = [partner, across] + [near(axis, by) for axis in EACH for by in AHEAD]
    barrier = pltpu.get_barrier_semaphore()
    for peer in peers:
        pl.semaphore_signal(barrier, inc=1, device_id={"dp": peer}, device_id_type=MESH)

    def start_all(what, ras, start=0):
        def body(j):
            for ra in ras:
                for i in EACH:
                    what(i, ra, order(j)).start()

        loop(body, start=start)

    def start_first(what):
        def body(c):
            for i in EACH:
                what(i, c).start()

        loop(body)

    start_first(first_load)
    start_all(load, (2,), 1)
    pl.semaphore_wait(barrier, len(peers))
    start_first(first_trade)
    start_all(trade, (2,), 1)
    for ras in (AHEAD, (0,)):
        start_all(load, ras)
        start_all(trade, ras)
    own = [
        pltpu.make_async_copy(wg.at[:, pos[0], pos[1], pos[2], k], own_g, own_sem.at[0]),
        pltpu.make_async_copy(wu.at[:, pos[0], pos[1], pos[2], k], own_u, own_sem.at[1]),
        pltpu.make_async_copy(wd.at[:, pos[0], pos[1], pos[2] // 2], own_d, own_sem.at[2]),
    ]
    for n, (moment, there) in enumerate(zip((mg, mu, md, vg, vu, vd), (mg2, mu2, md2, vg2, vu2, vd2))):
        own.append(pltpu.make_async_copy(moment, there, own_sem.at[3 + n]))
    for one in own:
        one.start()

    def sum0(i, l, a, b, c):
        return f32(at(i, l, a, b, c, k)[...]) + f32(at(i, l, a, b, c, 1 - k)[...])

    def sum1(i, l, b, c):
        return sum0(i, l, home[i][0], b, c) + f32(R2[i][0, l, b, c]) + f32(R2[i][1, l, b, c])

    def sum2(i, l, c):
        return sum1(i, l, home[i][1], c) + f32(Q2[i][0, l, c]) + f32(Q2[i][1, l, c])

    def hop_a(i, kind, rb):
        d, b = kind % 2, rel(i, B, rb)
        to = near(AXES[i][0], AHEAD[d])
        if kind < 2:
            src, dst = at(i, d, rel(i, A, FAR), b, ALL, k), R1[i].at[d, b]
        elif kind < 4:
            src, dst = at(i, 1 - d, rel(i, A, AHEAD[d]), b, ALL, k), R2[i].at[d, 1 - d, b]
        else:
            src, dst = R1[i].at[d, b], R2[i].at[d, d, b]
        return copy(src, dst, a_s.at[i, min(kind // 2, 1)], a_r.at[i, min(kind, 2), rb], to)

    def hop_b(i, kind, rc):
        d, c = kind % 2, rel(i, C, rc)
        to = near(AXES[i][1], AHEAD[d])
        if kind < 2:
            src, dst = R2[i].at[0, d, rel(i, B, FAR), c], Q1[i].at[d, c]
        elif kind < 4:
            src, dst = R2[i].at[0, 1 - d, rel(i, B, AHEAD[d]), c], Q2[i].at[d, 1 - d, c]
        else:
            src, dst = Q1[i].at[d, c], Q2[i].at[d, d, c]
        return copy(src, dst, b_s.at[i, min(kind // 2, 1)], b_r.at[i, min(kind, 2), rc], to)

    def hop_c(i, kind):
        d = kind % 2
        to = near(AXES[i][2], AHEAD[d])
        if kind < 2:
            src, dst = Q2[i].at[0, d, rel(i, C, FAR)], P1[i].at[d]
        elif kind < 4:
            src, dst = Q2[i].at[0, 1 - d, rel(i, C, AHEAD[d])], P2[i].at[d, 1 - d]
        else:
            src, dst = P1[i].at[d], P2[i].at[d, d]
        return copy(src, dst, c_s.at[i, min(kind // 2, 1)], c_r.at[i, min(kind, 2)], to)

    def farthest(j):
        rb = order(j)
        for i in EACH:
            traded(i, 2, rb)
            a, b = rel(i, A, FAR), rel(i, B, rb)

            def add(t):
                at(i, t // 4, a, b, lax.rem(t, 4), k)[...] = sum0(i, t // 4, a, b, lax.rem(t, 4)).astype(BF16)

            loop(add, 8)
            hop_a(i, 0, rb).start()
            hop_a(i, 1, rb).start()

    def farthest_first(c):
        for i in EACH:
            first_traded(i, c)
            a, b = rel(i, A, FAR), rel(i, B, FAR)
            for l in SIDES:
                ref = at(i, l, a, b, c, k)
                ref[...] = sum0(i, l, a, b, c).astype(BF16)
                copy(ref, R1[i].at[l, b, c], a_s.at[i, 0], a_r.at[i, l, 2], near(AXES[i][0], AHEAD[l])).start()

    loop(farthest_first)
    loop(farthest, start=1)

    def plain(j):
        rb = order(j)
        for i in EACH:
            for d in SIDES:
                ra = AHEAD[d]
                traded(i, ra, rb)
                a, b = rel(i, A, ra), rel(i, B, rb)

                def add(c):
                    at(i, 1 - d, a, b, c, k)[...] = sum0(i, 1 - d, a, b, c).astype(BF16)

                loop(add)
                hop_a(i, 2 + d, rb).start()

    loop(plain)

    def onward(j):
        rb = order(j)
        for i in EACH:
            for d in SIDES:
                hop_a(i, d, rb).wait_recv()
                a, b = rel(i, A, AHEAD[d]), rel(i, B, rb)

                def add(c):
                    R1[i][d, b, c] = (f32(R1[i][d, b, c]) + sum0(i, d, a, b, c)).astype(BF16)

                loop(add)
                hop_a(i, 4 + d, rb).start()

    loop(onward)

    def arrived_a(i, rb):
        traded(i, 0, rb)
        landed(R1[i].at[0], a_r.at[i, 2, rb])

    def settle_a(i, l, rb, rc):
        b, c = rel(i, B, rb), rel(i, C, rc)
        R2[i][0, l, b, c] = sum1(i, l, b, c).astype(BF16)

    for i in EACH:
        arrived_a(i, 2)

        def far_b(j, i=i):
            for d in SIDES:
                settle_a(i, d, 2, order(j))
                hop_b(i, d, order(j)).start()

        loop(far_b)
    for rb in AHEAD:
        for i in EACH:
            arrived_a(i, rb)

    def near_b(j):
        rc = order(j)
        for i in EACH:
            for d in SIDES:
                settle_a(i, 1 - d, AHEAD[d], rc)
                hop_b(i, 2 + d, rc).start()
        for i in EACH:
            for d in SIDES:
                hop_b(i, d, rc).wait_recv()
                c = rel(i, C, rc)
                Q1[i][d, c] = (f32(Q1[i][d, c]) + sum1(i, d, rel(i, B, AHEAD[d]), c)).astype(BF16)
                hop_b(i, 4 + d, rc).start()

    loop(near_b)
    for i in EACH:
        sent(R1[i], a_s.at[i, 0])
        sent(R2[i], a_s.at[i, 1])
        sent(at(i, ALL, ALL, ALL, ALL, k), d2d_s.at[i])
    for i in EACH:
        arrived_a(i, 0)

    def arrived_b(i, rc):
        landed(P2[i], b_r.at[i, 2, rc])

    for i in EACH:
        arrived_b(i, 2)
        for d in SIDES:
            c = rel(i, C, FAR)
            Q2[i][0, d, c] = sum2(i, d, c).astype(BF16)
            hop_c(i, d).start()
    for d in (1, 0):
        for i in EACH:
            arrived_b(i, AHEAD[d])
            c = rel(i, C, AHEAD[d])
            Q2[i][0, 1 - d, c] = sum2(i, 1 - d, c).astype(BF16)
            hop_c(i, 2 + d).start()
    for i in EACH:
        for d in SIDES:
            partial[i][d] = sum2(i, d, rel(i, C, AHEAD[d]))
    for i in EACH:
        sent(Q1[i], b_s.at[i, 0])
        sent(Q2[i], b_s.at[i, 1])
    for i in EACH:
        for d in SIDES:
            hop_c(i, d).wait_recv()
            P1[i][d] = (f32(P1[i][d]) + partial[i][d]).astype(BF16)
            hop_c(i, 4 + d).start()
    for i in EACH:
        arrived_b(i, 0)
        for l in SIDES:
            partial[i][l] = sum2(i, l, home[i][2])
    squares = jnp.zeros((8, 128), F32)
    for i in (2, 0, 1):
        landed(P2[i], c_r.at[i, 2])
        for l in SIDES:
            total = (partial[i][l] + f32(P2[i][0, l]) + f32(P2[i][1, l])).astype(BF16)
            if i == 2:
                quad_g[q, l] = total
            else:
                P2[i][0, l] = total
            s = f32(total)
            s = s * s
            if i == 2:
                s = jnp.sum(s, axis=0)
            for lane in range(0, s.shape[-1], 128):
                squares = squares + s[:, lane : lane + 128]
        if i == 2:
            for n in EACH:
                copy(quad_g.at[q], quad_g.at[q], x_s.at[n], x_r.at[n], quad[n]).start()
    norms[0, 0] = jnp.sum(squares, axis=0, keepdims=True)

    for i in EACH:
        sent(P1[i], c_s.at[i, 0])
        sent(P2[i], c_s.at[i, 1])

    line, plane = lax.rem(me, 8), me // 8
    def build_rows():
        for one in own:
            one.wait()
        for n in EACH:
            copy(quad_g.at[q], quad_g.at[q], x_s.at[n], x_r.at[n], quad[n]).wait_send()
            theirs = quad_g.at[lax.rem(q + n + 1, 4)]
            copy(theirs, theirs, x_s.at[2 - n], x_r.at[2 - n], quad[n]).wait_recv()
        for l in SIDES:
            for n in PLACES:
                rows[0, l, :, n * quarter : (n + 1) * quarter] = f32(quad_g[n, l]).reshape(4 * n_rows, quarter)
            rows[1, l] = f32(own_d[l]).reshape(4 * n_rows, 4 * quarter)

    n_rows = md.shape[0]
    for turn, others in ((0, [plane * 8 + lax.rem(line + by, 8) for by in range(1, 8)]), (1, [lax.rem(plane + by, 16) * 8 + line for by in range(1, 16)])):
        hops = [copy(norms.at[turn, 0], norms.at[turn, by], n_s.at[turn, by], n_r.at[turn, by], to) for by, to in enumerate(others, 1)]
        for hop in hops:
            hop.start()
        if turn == 1:
            build_rows()
        for hop in hops:
            hop.wait()
        squares = jnp.sum(norms[turn, 0 : len(hops) + 1], axis=0)
        if turn == 0:
            norms[1, 0] = squares
    squares = jnp.sum(squares, axis=1, keepdims=True)
    factor = jnp.minimum(1.0, 0.5 * lax.rsqrt(squares / count + 1e-30))

    def adamw(w, m, v, g):
        g = g * factor
        m = 0.9 * m + 0.1 * g
        v = 0.95 * v + 0.05 * g * g
        step = m * lax.rsqrt(v + 1e-8) + 0.1 * w
        return (w - 0.02 * step).astype(BF16), m, v

    def back_c(i, kind):
        d = kind % 2
        a, b, c = home[i]
        if kind < 2:
            ref = at(i, ALL, a, b, c, k)
        else:
            ref = at(i, d, a, b, rel(i, C, BEHIND[d]), k)
        return copy(ref, ref, c_s.at[i, 1 - kind // 2], c_r.at[i, min(kind, 2)], near(AXES[i][2], AHEAD[d]))

    def came_c(i, d):
        a, b, _ = home[i]
        landed(at(i, ALL, a, b, rel(i, C, BEHIND[d]), k), c_r.at[i, d])

    def back_b(i, kind):
        d = kind % 2
        a, b, _ = home[i]
        if kind < 2:
            ref = at(i, ALL, a, b, ALL, k)
        else:
            ref = at(i, d, a, rel(i, B, BEHIND[d]), ALL, k)
        return copy(ref, ref, b_s.at[i, 1 - kind // 2], b_r.at[i, min(kind, 2), 0], near(AXES[i][1], AHEAD[d]))

    def came_b(i, d):
        landed(at(i, ALL, home[i][0], rel(i, B, BEHIND[d]), ALL, k), b_r.at[i, d, 0])

    def back_a(i, kind, rb):
        d, b = kind % 2, rel(i, B, rb)
        if kind < 2:
            ref = at(i, ALL, home[i][0], b, ALL, k)
        else:
            ref = at(i, d, rel(i, A, BEHIND[d]), b, ALL, k)
        return copy(ref, ref, a_s.at[i, 1 - kind // 2], a_r.at[i, min(kind, 2), rb], near(AXES[i][0], AHEAD[d]))

    def came_a(i, d, rb):
        landed(at(i, ALL, rel(i, A, BEHIND[d]), rel(i, B, rb), ALL, k), a_r.at[i, d, rb])

    def share(i, ra, rb):
        ref = at(i, ALL, rel(i, A, ra), rel(i, B, rb), ALL, k)
        return copy(ref, ref, d2d_s.at[i], share_r.at[i], partner)

    def spread(i, c):
        a, b, _ = home[i]
        ref = at(i, ALL, a, b, c, k)
        for d in SIDES:
            copy(ref, ref, b_s.at[i, 1], b_r.at[i, d, 0], near(AXES[i][1], AHEAD[d])).start()
        for d in SIDES:
            copy(ref, ref, a_s.at[i, 1], a_r.at[i, d, 0], near(AXES[i][0], AHEAD[d])).start()

    def begin(i):
        for kind in SIDES:
            back_c(i, kind).start()
        spread(i, home[i][2])

    for i, own_w, m_ref, v_ref in ((0, own_g, mg2, vg2), (1, own_u, mu2, vu2)):
        for l in SIDES:
            new, m_ref[l], v_ref[l] = adamw(f32(own_w[l]), m_ref[l], v_ref[l], f32(P2[i][0, l]))
            at(i, l, *home[i], k)[...] = new
        begin(i)

    for l in SIDES:
        for n in PLACES:

            @pl.when(q == n)
            def _():
                mine = slice(n * n_rows, (n + 1) * n_rows)
                new, m, v = adamw(rows[1, l, mine, :], md2[:, l, :], vd2[:, l, :], rows[0, l, mine, :])
                new_rows[l] = new
                md2[:, l, :] = m
                vd2[:, l, :] = v
                cols[n, l] = new[:, n * quarter : (n + 1) * quarter]

    def piece(n):
        to = lax.rem(q + n + 1, 4)
        return new_rows.at[:, :, pl.ds(pl.multiple_of(to * quarter, quarter), quarter)]

    for n in EACH:
        copy(piece(n), cols.at[q], x_s.at[3 + n], x_r.at[3 + n], quad[n]).start()
    for n in EACH:
        copy(piece(n), cols.at[q], x_s.at[3 + n], x_r.at[3 + n], quad[n]).wait_send()
        theirs = cols.at[lax.rem(q + n + 1, 4)]
        copy(theirs, theirs, x_s.at[5 - n], x_r.at[5 - n], quad[n]).wait_recv()
    for l in SIDES:
        for n in PLACES:
            rows[0, l, n * n_rows : (n + 1) * n_rows, 0:quarter] = f32(cols[n, l])
        at(2, l, *home[2], k)[...] = rows[0, l, :, 0:quarter].reshape(n_rows // 2, 8, quarter).astype(BF16)
    begin(2)
    for i in EACH:
        for d in SIDES:
            came_c(i, d)
            back_c(i, 2 + d).start()
        for d in SIDES:
            spread(i, rel(i, C, AHEAD[d]))
    for i in EACH:
        landed(P1[i], c_r.at[i, 2])
        spread(i, rel(i, C, FAR))
        share(i, 0, 0).start()
    for i in EACH:
        for d in SIDES:
            came_b(i, d)
            back_b(i, 2 + d).start()
    for i in EACH:
        for rb in (3, 1):
            for kind in SIDES:
                back_a(i, kind, rb).start()
            share(i, 0, rb).start()
    for i in EACH:
        landed(Q1[i], b_r.at[i, 2, 0])
        for kind in SIDES:
            back_a(i, kind, 2).start()
        share(i, 0, 2).start()

    def pass_on(j):
        rb = lax.rem(order(j) + 2, 4)
        for i in EACH:
            for d in SIDES:
                came_a(i, d, rb)
                back_a(i, 2 + d, rb).start()
                share(i, BEHIND[d], rb).start()

    loop(pass_on, 3)

    def tail(i, d, c):
        ref = at(i, d, rel(i, A, BEHIND[d]), rel(i, B, FAR), c, k)
        return copy(ref, ref, a_s.at[i, 0], tail_r.at[i, c], near(AXES[i][0], AHEAD[d]))

    for i in EACH:
        for d in SIDES:
            came_a(i, d, 2)

    def pass_tail(c):
        for i in EACH:
            for d in SIDES:
                tail(i, d, c).start()

    loop(pass_tail)
    for i in EACH:
        for d in SIDES:
            share(i, BEHIND[d], 2).start()

    def last(j):
        rb = lax.rem(order(j) + 2, 4)
        for i in EACH:
            landed(Q1[i], a_r.at[i, 2, rb])
            share(i, 2, rb).start()

    loop(last, 3)

    def last_tail(c):
        for i in EACH:
            landed(P1[i], tail_r.at[i, c])
            ref = at(i, ALL, rel(i, A, FAR), rel(i, B, FAR), c, k)
            copy(ref, ref, d2d_s.at[i], share_r.at[i], partner).start()

    loop(last_tail)

    for i in EACH:
        sent(R1[i], a_s.at[i, 0])
        sent(R2[i], a_s.at[i, 1])
        sent(Q1[i], b_s.at[i, 0])
        sent(Q2[i], b_s.at[i, 1])
        sent(P1[i], c_s.at[i, 0])
        sent(P2[i], c_s.at[i, 1])
    for i in EACH:
        landed(at(i, ALL, ALL, ALL, ALL, 1 - k), share_r.at[i])
        sent(at(i, ALL, ALL, ALL, ALL, k), d2d_s.at[i])


def write_wide(n_wide, *refs):
    sems = refs[-1]
    copies = [
        pltpu.make_async_copy(W.at[l, n], out.at[l, n], sems.at[8 * i + 4 * l + n]) for i, (W, out) in enumerate(zip(refs[:n_wide], refs[n_wide:-1])) for l in SIDES for n in PLACES
    ]
    for one in copies:
        one.start()
    for one in copies:
        one.wait()


def write_tall(n_small, W, *refs):
    small_in, out, small_out, sems = refs[:n_small], refs[n_small], refs[n_small + 1 : -1], refs[-1]
    quarter = W.shape[-1]
    copies = [pltpu.make_async_copy(r, o, sems.at[n]) for n, (r, o) in enumerate(zip(small_in, small_out))]
    for n in PLACES:
        for half in SIDES:
            columns = slice(n * quarter, (n + 1) * quarter)
            copies.append(pltpu.make_async_copy(W.at[:, :, :, 2 * half + n // 2, n % 2], out.at[:, :, :, half, :, :, columns], sems.at[len(copies)]))
    for one in copies:
        one.start()
    for one in copies:
        one.wait()


def solution(mesh):
    def step(*arrays):
        terms, weights, m, v = (arrays[i : i + 3] for i in (0, 3, 6, 9))
        wide, tall = weights[0].shape[2], weights[2].shape[2]
        n_rows = m[2].shape[1]
        m, v = ([jnp.swapaxes(one, 0, 1) if n == 2 else one for n, one in enumerate(some)] for some in (m, v))
        whole = (LAYERS, 4, 4, 4, 2, 8, wide)
        whole_d = (LAYERS, 4, 4, 2, n_rows // 2, 8, tall)
        shapes = (whole, whole, whole_d)
        quarter = tall // 4
        units = ((8, wide), (8, wide), (n_rows // 2, 8, quarter))
        g = [t[0].reshape(s) for t, s in zip(terms, shapes)]
        w = [t.reshape(s) for t, s in zip(weights, shapes)]
        count = float(sum(one.size for one in weights))
        blocks = [pltpu.VMEM((LAYERS, 4, 4, 4, 2, *u), BF16) for u in units]
        moments = [pltpu.VMEM(one.shape, F32) for one in (*m, *v)]
        hbm, vmem = pl.BlockSpec(memory_space=pltpu.HBM), pl.BlockSpec(memory_space=pltpu.VMEM)
        dma = pltpu.SemaphoreType.DMA
        results = pl.pallas_call(
            functools.partial(step_kernel, count),
            out_shape=blocks + moments,
            in_specs=[hbm] * 12,
            out_specs=[vmem] * 9,
            scratch_shapes=[
                *[pltpu.VMEM((2, 4, 4, *u), BF16) for u in units],
                *[pltpu.VMEM((2, LAYERS, 4, 4, *u), BF16) for u in units],
                *[pltpu.VMEM((2, 4, *u), BF16) for u in units],
                *[pltpu.VMEM((2, LAYERS, 4, *u), BF16) for u in units],
                *[pltpu.VMEM((2, *u), BF16) for u in units],
                *[pltpu.VMEM((2, LAYERS, *u), BF16) for u in units],
                *[pltpu.VMEM((LAYERS, *u), F32) for u in units],
                pltpu.VMEM((LAYERS, 8, wide), BF16),
                pltpu.VMEM((LAYERS, 8, wide), BF16),
                pltpu.VMEM((LAYERS, n_rows // 2, 8, tall), BF16),
                pltpu.VMEM((4, LAYERS, *units[2]), BF16),
                pltpu.VMEM((2, LAYERS, 4 * n_rows, tall), F32),
                pltpu.VMEM((LAYERS, n_rows, tall), BF16),
                pltpu.VMEM((4, LAYERS, n_rows, quarter), BF16),
                pltpu.VMEM((2, 16, 1, 128), F32),
                dma((3, 4, 4)), dma((9,)), dma((3,)), dma((3, 4, 4)),
                dma((3, 2)), dma((3, 3, 4)), dma((3, 2)), dma((3, 3, 4)), dma((3, 2)), dma((3, 3)),
                dma((6,)), dma((6,)), dma((2, 16)), dma((2, 16)), dma((3, 4)), dma((3, 4)), dma((3, 4)), dma((3,)),
            ],
            compiler_params=pltpu.CompilerParams(collective_id=0, has_side_effects=True, vmem_limit_bytes=26600000),
            name="step",
        )(*g, *w, *m, *v)

        def write(kernel, arrays, outs):
            return pl.pallas_call(
                kernel,
                out_shape=outs,
                in_specs=[vmem] * len(arrays),
                out_specs=[hbm] * len(outs),
                scratch_shapes=[dma((16,))],
                compiler_params=pltpu.CompilerParams(vmem_limit_bytes=2**20),
                name="write",
            )(*arrays)

        outs = [jax.ShapeDtypeStruct(s, BF16) for s in shapes]
        small = results[3:]
        new_gate, new_up = write(functools.partial(write_wide, 2), results[:2], outs[:2])
        new_down, *moved = write(functools.partial(write_tall, len(small)), results[2:], outs[2:] + [jax.ShapeDtypeStruct(one.shape, F32) for one in small])
        new = [r.reshape(t.shape) for r, t in zip((new_gate, new_up, new_down), weights)]
        return (*new, *(jnp.swapaxes(one, 0, 1) if n % 3 == 2 else one for n, one in enumerate(moved)))

    all_of, cut = P(None, None, None), P(None, "dp", None)
    return jax.shard_map(
        step,
        mesh=mesh,
        in_specs=(P(("rep", "dp"), None, None, None),) * 3 + (all_of,) * 3 + (cut,) * 6,
        out_specs=(P("rep", None, None),) * 3 + (P("rep", "dp", None),) * 6,
        check_vma=False,
    )
```

```python
import functools

import jax
import jax.numpy as jnp
from jax import lax
from jax.experimental import pallas as pl
from jax.experimental.pallas import tpu as pltpu
from jax.sharding import PartitionSpec as P

MESH = pl.DeviceIdType.MESH
F32, BF16 = jnp.float32, jnp.bfloat16
AXES = ((0, 1, 2), (1, 2, 0), (2, 0, 1))
LAYERS = 2
A, B, C = range(3)
FAR = 2
EACH, SIDES, PLACES, OTHERS, LANDED = range(3), range(2), range(4), range(1, 4), range(2, 6)
AHEAD, BEHIND = (1, 3), (3, 1)


def order(j):
    return lax.rem(2 + j + lax.div(j, 2) * (2 * j - 3), 4)


def loop(body, n=4, start=0):
    lax.fori_loop(start, n, lambda j, c: (body(j), c)[1], 0)


def f32(x):
    return x.astype(F32)


def step_kernel(
    count, gg, gu, gd, wg, wu, wd, mg, mu, md, vg, vu, vd,
    Wg, Wu, Wd, mg2, mu2, md2, vg2, vu2, vd2,
    R1g, R1u, R1d, R2g, R2u, R2d, Q1g, Q1u, Q1d, Q2g, Q2u, Q2d, P1g, P1u, P1d, P2g, P2u, P2d,
    partial_g, partial_u, partial_d, own_g, own_u, own_d, quad_g, rows, new_rows, cols, norms,
    load_sem, own_sem, d2d_s, d2d_r, a_s, a_r, b_s, b_r, c_s, c_r, x_s, x_r, n_s, n_r, piece_l, piece_r, tail_r, share_r,
):
    g_in, W, w_in = (gg, gu, gd), (Wg, Wu, Wd), (wg, wu, wd)
    R1, R2, Q1, Q2, P1, P2 = (R1g, R1u, R1d), (R2g, R2u, R2d), (Q1g, Q1u, Q1d), (Q2g, Q2u, Q2d), (P1g, P1u, P1d), (P2g, P2u, P2d)
    partial = (partial_g, partial_u, partial_d)
    quarter = cols.shape[-1]
    me = lax.axis_index("dp")
    k = lax.rem(me, 2)
    pos = (me // 32, lax.rem(me // 8, 4), lax.rem(me // 2, 4))
    q = lax.rem(me, 4)

    def device(p, core):
        return ((p[0] * 4 + p[1]) * 4 + p[2]) * 2 + core

    def near(axis, by):
        return device([lax.rem(c + by, 4) if n == axis else c for n, c in enumerate(pos)], k)

    partner = device(pos, 1 - k)
    quad = [me - q + lax.rem(q + by, 4) for by in OTHERS]

    def copy(src, dst, send, recv, to):
        return pltpu.make_async_remote_copy(src_ref=src, dst_ref=dst, send_sem=send, recv_sem=recv, device_id={"dp": to}, device_id_type=MESH)

    def at(i, l, a, b, c, core):
        place = dict(zip(AXES[i], (a, b, c)))
        return W[i].at[l, place[0], place[1], place[2], core]

    ALL = slice(None)
    home = [[pos[n] for n in AXES[i]] for i in EACH]

    around = [[lax.rem(one + by, 4) for by in PLACES] for one in pos]

    def rel(i, which, by):
        if isinstance(by, int):
            return around[AXES[i][which]][by]
        return lax.rem(home[i][which] + by, 4)

    def sent(ref, sem):
        copy(ref, ref, sem, x_r.at[0], partner).wait_send()

    def landed(ref, sem):
        copy(ref, ref, x_s.at[0], sem, partner).wait_recv()

    def source(i, a, b, c, core):
        if i == 0:
            return gg.at[:, a, b, c, core]
        if i == 1:
            return gu.at[:, c, a, b, core]
        columns = pl.ds(pl.multiple_of(lax.rem(a, 2) * (2 * quarter) + core * quarter, quarter), quarter)
        return gd.at[:, b, c, a // 2, :, :, columns]

    def load(i, ra, rb):
        a, b = rel(i, A, ra), rel(i, B, rb)
        return pltpu.make_async_copy(source(i, a, b, ALL, k), at(i, ALL, a, b, ALL, k), load_sem.at[i, ra, rb])

    def trade(i, ra, rb):
        a, b = rel(i, A, ra), rel(i, B, rb)
        return copy(source(i, a, b, ALL, 1 - k), at(i, ALL, a, b, ALL, k), d2d_s.at[i], d2d_r.at[i, ra, rb], partner)

    def first_load(i, c):
        a, b = rel(i, A, FAR), rel(i, B, FAR)
        return pltpu.make_async_copy(source(i, a, b, c, k), at(i, ALL, a, b, c, k), piece_l.at[i, c])

    def first_trade(i, c):
        a, b = rel(i, A, FAR), rel(i, B, FAR)
        return copy(source(i, a, b, c, 1 - k), at(i, ALL, a, b, c, k), d2d_s.at[i], piece_r.at[i, c], partner)

    def first_traded(i, c):
        a, b = rel(i, A, FAR), rel(i, B, FAR)
        first_load(i, c).wait()
        ref = at(i, ALL, a, b, c, 1 - k)
        copy(ref, ref, d2d_s.at[i], piece_r.at[i, c], partner).wait_recv()

    def traded(i, ra, rb):
        a, b = rel(i, A, ra), rel(i, B, rb)
        load(i, ra, rb).wait()
        copy(at(i, ALL, a, b, ALL, 1 - k), at(i, ALL, a, b, ALL, 1 - k), d2d_s.at[i], d2d_r.at[i, ra, rb], partner).wait_recv()

    across = me - q + (2 - 2 * (q // 2)) + (1 - k)
    peers = [partner, across] + [near(axis, by) for axis in EACH for by in AHEAD]
    barrier = pltpu.get_barrier_semaphore()
    for peer in peers:
        pl.semaphore_signal(barrier, inc=1, device_id={"dp": peer}, device_id_type=MESH)

    def start_all(what, ras, start=0):
        def body(j):
            for ra in ras:
                for i in EACH:
                    what(i, ra, order(j)).start()

        loop(body, start=start)

    def start_first(what):
        def body(c):
            for i in EACH:
                what(i, c).start()

        loop(body)

    start_first(first_load)
    start_all(load, (2,), 1)
    pl.semaphore_wait(barrier, len(peers))
    start_first(first_trade)
    start_all(trade, (2,), 1)
    for ras in (AHEAD, (0,)):
        start_all(load, ras)
        start_all(trade, ras)
    own = [
        pltpu.make_async_copy(wg.at[:, pos[0], pos[1], pos[2], k], own_g, own_sem.at[0]),
        pltpu.make_async_copy(wu.at[:, pos[0], pos[1], pos[2], k], own_u, own_sem.at[1]),
        pltpu.make_async_copy(wd.at[:, pos[0], pos[1], pos[2] // 2], own_d, own_sem.at[2]),
    ]
    for n, (moment, there) in enumerate(zip((mg, mu, md, vg, vu, vd), (mg2, mu2, md2, vg2, vu2, vd2))):
        own.append(pltpu.make_async_copy(moment, there, own_sem.at[3 + n]))
    for one in own:
        one.start()

    def sum0(i, l, a, b, c):
        return f32(at(i, l, a, b, c, k)[...]) + f32(at(i, l, a, b, c, 1 - k)[...])

    def sum1(i, l, b, c):
        return sum0(i, l, home[i][0], b, c) + f32(R2[i][0, l, b, c]) + f32(R2[i][1, l, b, c])

    def sum2(i, l, c):
        return sum1(i, l, home[i][1], c) + f32(Q2[i][0, l, c]) + f32(Q2[i][1, l, c])

    def hop_a(i, kind, rb):
        d, b = kind % 2, rel(i, B, rb)
        to = near(AXES[i][0], AHEAD[d])
        if kind < 2:
            src, dst = at(i, d, rel(i, A, FAR), b, ALL, k), R1[i].at[d, b]
        elif kind < 4:
            src, dst = at(i, 1 - d, rel(i, A, AHEAD[d]), b, ALL, k), R2[i].at[d, 1 - d, b]
        else:
            src, dst = R1[i].at[d, b], R2[i].at[d, d, b]
        return copy(src, dst, a_s.at[i, min(kind // 2, 1)], a_r.at[i, min(kind, 2), rb], to)

    def hop_b(i, kind, rc):
        d, c = kind % 2, rel(i, C, rc)
        to = near(AXES[i][1], AHEAD[d])
        if kind < 2:
            src, dst = R2[i].at[0, d, rel(i, B, FAR), c], Q1[i].at[d, c]
        elif kind < 4:
            src, dst = R2[i].at[0, 1 - d, rel(i, B, AHEAD[d]), c], Q2[i].at[d, 1 - d, c]
        else:
            src, dst = Q1[i].at[d, c], Q2[i].at[d, d, c]
        return copy(src, dst, b_s.at[i, min(kind // 2, 1)], b_r.at[i, min(kind, 2), rc], to)

    def hop_c(i, kind):
        d = kind % 2
        to = near(AXES[i][2], AHEAD[d])
        if kind < 2:
            src, dst = Q2[i].at[0, d, rel(i, C, FAR)], P1[i].at[d]
        elif kind < 4:
            src, dst = Q2[i].at[0, 1 - d, rel(i, C, AHEAD[d])], P2[i].at[d, 1 - d]
        else:
            src, dst = P1[i].at[d], P2[i].at[d, d]
        return copy(src, dst, c_s.at[i, min(kind // 2, 1)], c_r.at[i, min(kind, 2)], to)

    def farthest(j):
        rb = order(j)
        for i in EACH:
            traded(i, 2, rb)
            a, b = rel(i, A, FAR), rel(i, B, rb)

            def add(t):
                at(i, t // 4, a, b, lax.rem(t, 4), k)[...] = sum0(i, t // 4, a, b, lax.rem(t, 4)).astype(BF16)

            loop(add, 8)
            hop_a(i, 0, rb).start()
            hop_a(i, 1, rb).start()

    def farthest_first(c):
        for i in EACH:
            first_traded(i, c)
            a, b = rel(i, A, FAR), rel(i, B, FAR)
            for l in SIDES:
                ref = at(i, l, a, b, c, k)
                ref[...] = sum0(i, l, a, b, c).astype(BF16)
                copy(ref, R1[i].at[l, b, c], a_s.at[i, 0], a_r.at[i, l, 2], near(AXES[i][0], AHEAD[l])).start()

    loop(farthest_first)
    loop(farthest, start=1)

    def plain(j):
        rb = order(j)
        for i in EACH:
            for d in SIDES:
                ra = AHEAD[d]
                traded(i, ra, rb)
                a, b = rel(i, A, ra), rel(i, B, rb)

                def add(c):
                    at(i, 1 - d, a, b, c, k)[...] = sum0(i, 1 - d, a, b, c).astype(BF16)

                loop(add)
                hop_a(i, 2 + d, rb).start()

    loop(plain)

    def onward(j):
        rb = order(j)
        for i in EACH:
            for d in SIDES:
                hop_a(i, d, rb).wait_recv()
                a, b = rel(i, A, AHEAD[d]), rel(i, B, rb)

                def add(c):
                    R1[i][d, b, c] = (f32(R1[i][d, b, c]) + sum0(i, d, a, b, c)).astype(BF16)

                loop(add)
                hop_a(i, 4 + d, rb).start()

    loop(onward)

    def arrived_a(i, rb):
        traded(i, 0, rb)
        landed(R1[i].at[0], a_r.at[i, 2, rb])

    def settle_a(i, l, rb, rc):
        b, c = rel(i, B, rb), rel(i, C, rc)
        R2[i][0, l, b, c] = sum1(i, l, b, c).astype(BF16)

    for i in EACH:
        arrived_a(i, 2)

        def far_b(j, i=i):
            for d in SIDES:
                settle_a(i, d, 2, order(j))
                hop_b(i, d, order(j)).start()

        loop(far_b)
    for rb in AHEAD:
        for i in EACH:
            arrived_a(i, rb)

    def near_b(j):
        rc = order(j)
        for i in EACH:
            for d in SIDES:
                settle_a(i, 1 - d, AHEAD[d], rc)
                hop_b(i, 2 + d, rc).start()
        for i in EACH:
            for d in SIDES:
                hop_b(i, d, rc).wait_recv()
                c = rel(i, C, rc)
                Q1[i][d, c] = (f32(Q1[i][d, c]) + sum1(i, d, rel(i, B, AHEAD[d]), c)).astype(BF16)
                hop_b(i, 4 + d, rc).start()

    loop(near_b)
    for i in EACH:
        sent(R1[i], a_s.at[i, 0])
        sent(R2[i], a_s.at[i, 1])
        sent(at(i, ALL, ALL, ALL, ALL, k), d2d_s.at[i])
    for i in EACH:
        arrived_a(i, 0)

    def arrived_b(i, rc):
        landed(P2[i], b_r.at[i, 2, rc])

    for i in EACH:
        arrived_b(i, 2)
        for d in SIDES:
            c = rel(i, C, FAR)
            Q2[i][0, d, c] = sum2(i, d, c).astype(BF16)
            hop_c(i, d).start()
    for d in (1, 0):
        for i in EACH:
            arrived_b(i, AHEAD[d])
            c = rel(i, C, AHEAD[d])
            Q2[i][0, 1 - d, c] = sum2(i, 1 - d, c).astype(BF16)
            hop_c(i, 2 + d).start()
    for i in EACH:
        for d in SIDES:
            partial[i][d] = sum2(i, d, rel(i, C, AHEAD[d]))
    for i in EACH:
        sent(Q1[i], b_s.at[i, 0])
        sent(Q2[i], b_s.at[i, 1])
    for i in EACH:
        for d in SIDES:
            hop_c(i, d).wait_recv()
            P1[i][d] = (f32(P1[i][d]) + partial[i][d]).astype(BF16)
            hop_c(i, 4 + d).start()
    for i in EACH:
        arrived_b(i, 0)
        for l in SIDES:
            partial[i][l] = sum2(i, l, home[i][2])
    squares = jnp.zeros((8, 128), F32)
    for i in (2, 0, 1):
        landed(P2[i], c_r.at[i, 2])
        for l in SIDES:
            total = (partial[i][l] + f32(P2[i][0, l]) + f32(P2[i][1, l])).astype(BF16)
            if i == 2:
                quad_g[q, l] = total
            else:
                P2[i][0, l] = total
            s = f32(total)
            s = s * s
            if i == 2:
                s = jnp.sum(s, axis=0)
            for lane in range(0, s.shape[-1], 128):
                squares = squares + s[:, lane : lane + 128]
        if i == 2:
            for n in EACH:
                copy(quad_g.at[q], quad_g.at[q], x_s.at[n], x_r.at[n], quad[n]).start()
    norms[0, 0] = jnp.sum(squares, axis=0, keepdims=True)

    for i in EACH:
        sent(P1[i], c_s.at[i, 0])
        sent(P2[i], c_s.at[i, 1])

    line, plane = lax.rem(me, 8), me // 8
    def build_rows():
        for one in own:
            one.wait()
        for n in EACH:
            copy(quad_g.at[q], quad_g.at[q], x_s.at[n], x_r.at[n], quad[n]).wait_send()
            theirs = quad_g.at[lax.rem(q + n + 1, 4)]
            copy(theirs, theirs, x_s.at[2 - n], x_r.at[2 - n], quad[n]).wait_recv()
        for l in SIDES:
            for n in PLACES:
                rows[0, l, :, n * quarter : (n + 1) * quarter] = f32(quad_g[n, l]).reshape(4 * n_rows, quarter)
            rows[1, l] = f32(own_d[l]).reshape(4 * n_rows, 4 * quarter)

    n_rows = md.shape[0]
    for turn, others in ((0, [plane * 8 + lax.rem(line + by, 8) for by in range(1, 8)]), (1, [lax.rem(plane + by, 16) * 8 + line for by in range(1, 16)])):
        hops = [copy(norms.at[turn, 0], norms.at[turn, by], n_s.at[turn, by], n_r.at[turn, by], to) for by, to in enumerate(others, 1)]
        for hop in hops:
            hop.start()
        if turn == 1:
            build_rows()
        for hop in hops:
            hop.wait()
        squares = jnp.sum(norms[turn, 0 : len(hops) + 1], axis=0)
        if turn == 0:
            norms[1, 0] = squares
    squares = jnp.sum(squares, axis=1, keepdims=True)
    factor = jnp.minimum(1.0, 0.5 * lax.rsqrt(squares / count + 1e-30))

    def adamw(w, m, v, g):
        g = g * factor
        m = 0.9 * m + 0.1 * g
        v = 0.95 * v + 0.05 * g * g
        step = m * lax.rsqrt(v + 1e-8) + 0.1 * w
        return (w - 0.02 * step).astype(BF16), m, v

    def back_c(i, kind):
        d = kind % 2
        a, b, c = home[i]
        if kind < 2:
            ref = at(i, ALL, a, b, c, k)
        else:
            ref = at(i, d, a, b, rel(i, C, BEHIND[d]), k)
        return copy(ref, ref, c_s.at[i, 1 - kind // 2], c_r.at[i, min(kind, 2)], near(AXES[i][2], AHEAD[d]))

    def came_c(i, d):
        a, b, _ = home[i]
        landed(at(i, ALL, a, b, rel(i, C, BEHIND[d]), k), c_r.at[i, d])

    def back_b(i, kind):
        d = kind % 2
        a, b, _ = home[i]
        if kind < 2:
            ref = at(i, ALL, a, b, ALL, k)
        else:
            ref = at(i, d, a, rel(i, B, BEHIND[d]), ALL, k)
        return copy(ref, ref, b_s.at[i, 1 - kind // 2], b_r.at[i, min(kind, 2), 0], near(AXES[i][1], AHEAD[d]))

    def came_b(i, d):
        landed(at(i, ALL, home[i][0], rel(i, B, BEHIND[d]), ALL, k), b_r.at[i, d, 0])

    def back_a(i, kind, rb):
        d, b = kind % 2, rel(i, B, rb)
        if kind < 2:
            ref = at(i, ALL, home[i][0], b, ALL, k)
        else:
            ref = at(i, d, rel(i, A, BEHIND[d]), b, ALL, k)
        return copy(ref, ref, a_s.at[i, 1 - kind // 2], a_r.at[i, min(kind, 2), rb], near(AXES[i][0], AHEAD[d]))

    def came_a(i, d, rb):
        landed(at(i, ALL, rel(i, A, BEHIND[d]), rel(i, B, rb), ALL, k), a_r.at[i, d, rb])

    def share(i, ra, rb):
        ref = at(i, ALL, rel(i, A, ra), rel(i, B, rb), ALL, k)
        return copy(ref, ref, d2d_s.at[i], share_r.at[i], partner)

    def spread(i, c):
        a, b, _ = home[i]
        ref = at(i, ALL, a, b, c, k)
        for d in SIDES:
            copy(ref, ref, b_s.at[i, 1], b_r.at[i, d, 0], near(AXES[i][1], AHEAD[d])).start()
        for d in SIDES:
            copy(ref, ref, a_s.at[i, 1], a_r.at[i, d, 0], near(AXES[i][0], AHEAD[d])).start()

    def begin(i):
        for kind in SIDES:
            back_c(i, kind).start()
        spread(i, home[i][2])

    for l in SIDES:
        for n in PLACES:

            @pl.when(q == n)
            def _():
                mine = slice(n * n_rows, (n + 1) * n_rows)
                new, m, v = adamw(rows[1, l, mine, :], md2[:, l, :], vd2[:, l, :], rows[0, l, mine, :])
                new_rows[l] = new
                md2[:, l, :] = m
                vd2[:, l, :] = v
                cols[n, l] = new[:, n * quarter : (n + 1) * quarter]

    def piece(n):
        to = lax.rem(q + n + 1, 4)
        return new_rows.at[:, :, pl.ds(pl.multiple_of(to * quarter, quarter), quarter)]

    for n in EACH:
        copy(piece(n), cols.at[q], x_s.at[3 + n], x_r.at[3 + n], quad[n]).start()
    for i, own_w, m_ref, v_ref in ((0, own_g, mg2, vg2), (1, own_u, mu2, vu2)):
        for l in SIDES:
            new, m_ref[l], v_ref[l] = adamw(f32(own_w[l]), m_ref[l], v_ref[l], f32(P2[i][0, l]))
            at(i, l, *home[i], k)[...] = new
        begin(i)

    for n in EACH:
        copy(piece(n), cols.at[q], x_s.at[3 + n], x_r.at[3 + n], quad[n]).wait_send()
        theirs = cols.at[lax.rem(q + n + 1, 4)]
        copy(theirs, theirs, x_s.at[5 - n], x_r.at[5 - n], quad[n]).wait_recv()
    for l in SIDES:
        for n in PLACES:
            rows[0, l, n * n_rows : (n + 1) * n_rows, 0:quarter] = f32(cols[n, l])
        at(2, l, *home[2], k)[...] = rows[0, l, :, 0:quarter].reshape(n_rows // 2, 8, quarter).astype(BF16)
    begin(2)
    for i in EACH:
        for d in SIDES:
            came_c(i, d)
            back_c(i, 2 + d).start()
        for d in SIDES:
            spread(i, rel(i, C, AHEAD[d]))
    for i in EACH:
        landed(P1[i], c_r.at[i, 2])
        spread(i, rel(i, C, FAR))
        share(i, 0, 0).start()
    for i in EACH:
        for d in SIDES:
            came_b(i, d)
            back_b(i, 2 + d).start()
    for i in EACH:
        for rb in (3, 1):
            for kind in SIDES:
                back_a(i, kind, rb).start()
            share(i, 0, rb).start()
    for i in EACH:
        landed(Q1[i], b_r.at[i, 2, 0])
        for kind in SIDES:
            back_a(i, kind, 2).start()
        share(i, 0, 2).start()

    def pass_on(j):
        rb = lax.rem(order(j) + 2, 4)
        for i in EACH:
            for d in SIDES:
                came_a(i, d, rb)
                back_a(i, 2 + d, rb).start()
                share(i, BEHIND[d], rb).start()

    loop(pass_on, 3)

    def tail(i, d, c):
        ref = at(i, d, rel(i, A, BEHIND[d]), rel(i, B, FAR), c, k)
        return copy(ref, ref, a_s.at[i, 0], tail_r.at[i, c], near(AXES[i][0], AHEAD[d]))

    for i in EACH:
        for d in SIDES:
            came_a(i, d, 2)

    def pass_tail(c):
        for i in EACH:
            for d in SIDES:
                tail(i, d, c).start()

    loop(pass_tail)
    for i in EACH:
        for d in SIDES:
            share(i, BEHIND[d], 2).start()

    def last(j):
        rb = lax.rem(order(j) + 2, 4)
        for i in EACH:
            landed(Q1[i], a_r.at[i, 2, rb])
            share(i, 2, rb).start()

    loop(last, 3)

    def last_tail(c):
        for i in EACH:
            landed(P1[i], tail_r.at[i, c])
            ref = at(i, ALL, rel(i, A, FAR), rel(i, B, FAR), c, k)
            copy(ref, ref, d2d_s.at[i], share_r.at[i], partner).start()

    loop(last_tail)

    for i in EACH:
        sent(R1[i], a_s.at[i, 0])
        sent(R2[i], a_s.at[i, 1])
        sent(Q1[i], b_s.at[i, 0])
        sent(Q2[i], b_s.at[i, 1])
        sent(P1[i], c_s.at[i, 0])
        sent(P2[i], c_s.at[i, 1])
    for i in EACH:
        landed(at(i, ALL, ALL, ALL, ALL, 1 - k), share_r.at[i])
        sent(at(i, ALL, ALL, ALL, ALL, k), d2d_s.at[i])


def write_wide(n_wide, *refs):
    sems = refs[-1]
    copies = [
        pltpu.make_async_copy(W.at[l, n], out.at[l, n], sems.at[8 * i + 4 * l + n]) for i, (W, out) in enumerate(zip(refs[:n_wide], refs[n_wide:-1])) for l in SIDES for n in PLACES
    ]
    for one in copies:
        one.start()
    for one in copies:
        one.wait()


def write_tall(n_small, W, *refs):
    small_in, out, small_out, sems = refs[:n_small], refs[n_small], refs[n_small + 1 : -1], refs[-1]
    quarter = W.shape[-1]
    copies = [pltpu.make_async_copy(r, o, sems.at[n]) for n, (r, o) in enumerate(zip(small_in, small_out))]
    for n in PLACES:
        for half in SIDES:
            columns = slice(n * quarter, (n + 1) * quarter)
            copies.append(pltpu.make_async_copy(W.at[:, :, :, 2 * half + n // 2, n % 2], out.at[:, :, :, half, :, :, columns], sems.at[len(copies)]))
    for one in copies:
        one.start()
    for one in copies:
        one.wait()


def solution(mesh):
    def step(*arrays):
        terms, weights, m, v = (arrays[i : i + 3] for i in (0, 3, 6, 9))
        wide, tall = weights[0].shape[2], weights[2].shape[2]
        n_rows = m[2].shape[1]
        m, v = ([jnp.swapaxes(one, 0, 1) if n == 2 else one for n, one in enumerate(some)] for some in (m, v))
        whole = (LAYERS, 4, 4, 4, 2, 8, wide)
        whole_d = (LAYERS, 4, 4, 2, n_rows // 2, 8, tall)
        shapes = (whole, whole, whole_d)
        quarter = tall // 4
        units = ((8, wide), (8, wide), (n_rows // 2, 8, quarter))
        g = [t[0].reshape(s) for t, s in zip(terms, shapes)]
        w = [t.reshape(s) for t, s in zip(weights, shapes)]
        count = float(sum(one.size for one in weights))
        blocks = [pltpu.VMEM((LAYERS, 4, 4, 4, 2, *u), BF16) for u in units]
        moments = [pltpu.VMEM(one.shape, F32) for one in (*m, *v)]
        hbm, vmem = pl.BlockSpec(memory_space=pltpu.HBM), pl.BlockSpec(memory_space=pltpu.VMEM)
        dma = pltpu.SemaphoreType.DMA
        results = pl.pallas_call(
            functools.partial(step_kernel, count),
            out_shape=blocks + moments,
            in_specs=[hbm] * 12,
            out_specs=[vmem] * 9,
            scratch_shapes=[
                *[pltpu.VMEM((2, 4, 4, *u), BF16) for u in units],
                *[pltpu.VMEM((2, LAYERS, 4, 4, *u), BF16) for u in units],
                *[pltpu.VMEM((2, 4, *u), BF16) for u in units],
                *[pltpu.VMEM((2, LAYERS, 4, *u), BF16) for u in units],
                *[pltpu.VMEM((2, *u), BF16) for u in units],
                *[pltpu.VMEM((2, LAYERS, *u), BF16) for u in units],
                *[pltpu.VMEM((LAYERS, *u), F32) for u in units],
                pltpu.VMEM((LAYERS, 8, wide), BF16),
                pltpu.VMEM((LAYERS, 8, wide), BF16),
                pltpu.VMEM((LAYERS, n_rows // 2, 8, tall), BF16),
                pltpu.VMEM((4, LAYERS, *units[2]), BF16),
                pltpu.VMEM((2, LAYERS, 4 * n_rows, tall), F32),
                pltpu.VMEM((LAYERS, n_rows, tall), BF16),
                pltpu.VMEM((4, LAYERS, n_rows, quarter), BF16),
                pltpu.VMEM((2, 16, 1, 128), F32),
                dma((3, 4, 4)), dma((9,)), dma((3,)), dma((3, 4, 4)),
                dma((3, 2)), dma((3, 3, 4)), dma((3, 2)), dma((3, 3, 4)), dma((3, 2)), dma((3, 3)),
                dma((6,)), dma((6,)), dma((2, 16)), dma((2, 16)), dma((3, 4)), dma((3, 4)), dma((3, 4)), dma((3,)),
            ],
            compiler_params=pltpu.CompilerParams(collective_id=0, has_side_effects=True, vmem_limit_bytes=26600000),
            name="step",
        )(*g, *w, *m, *v)

        def write(kernel, arrays, outs):
            return pl.pallas_call(
                kernel,
                out_shape=outs,
                in_specs=[vmem] * len(arrays),
                out_specs=[hbm] * len(outs),
                scratch_shapes=[dma((16,))],
                compiler_params=pltpu.CompilerParams(vmem_limit_bytes=2**20),
                name="write",
            )(*arrays)

        outs = [jax.ShapeDtypeStruct(s, BF16) for s in shapes]
        small = results[3:]
        new_gate, new_up = write(functools.partial(write_wide, 2), results[:2], outs[:2])
        new_down, *moved = write(functools.partial(write_tall, len(small)), results[2:], outs[2:] + [jax.ShapeDtypeStruct(one.shape, F32) for one in small])
        new = [r.reshape(t.shape) for r, t in zip((new_gate, new_up, new_down), weights)]
        return (*new, *(jnp.swapaxes(one, 0, 1) if n % 3 == 2 else one for n, one in enumerate(moved)))

    all_of, cut = P(None, None, None), P(None, "dp", None)
    return jax.shard_map(
        step,
        mesh=mesh,
        in_specs=(P(("rep", "dp"), None, None, None),) * 3 + (all_of,) * 3 + (cut,) * 6,
        out_specs=(P("rep", None, None),) * 3 + (P("rep", "dp", None),) * 6,
        check_vma=False,
    )
```
